256 devices in a mesh: prow: 8 (over z), pcol: 32 (over y, x, core).
Axes of the slice: x: 4, y: 4, z: 8, core: 2. Of those that a mesh axis runs over, the one named last changes fastest.
Arguments:
- points: float32 [1, 32, 2, 1024], P(None, 'pcol'), may hold values from 0 to 1
- range_length: float32 [1], replicated, may hold values from 0.05 to 0.15
- smoothness: int32 [1], replicated, may hold values from 0 to 2
- sketch_bank: bfloat16 [32, 48, 1024], P('pcol'), may hold values from -6 to 6
- sketch_ids: int32 [4, 8, 1, 32], P(None, 'prow', None, 'pcol'), may hold values from 0 to 31
- tile_ranks: int32 [4, 8, 1, 32], P(None, 'prow', None, 'pcol'), may hold values from 16 to 48
Outputs:
- y_factors: float32 [4, 8, 1, 32, 48, 1024], P(None, 'prow', None, 'pcol')
- c_factors: float32 [4, 8, 1, 32, 48, 1024], P(None, 'prow', None, 'pcol')
- tile_error: float32 [4, 8, 1, 32], P(None, 'prow', None, 'pcol')
- rank_total: int32 [1], replicated
The draws below stay inside these ranges and needn't reach their ends.
All inputs are finite; a program needn't handle non-finite values.
Results may differ from the reference program's by a relative error of at most 0.0098.
The reference program's roundings to bfloat16 on the way count: a program that leaves them out, or rounds other values in their place, can miss the bound.
Values may be sent and summed in bfloat16 or wider, within the bound.
No kernel may reach another device: no remote copies, remote signals or barrier semaphores. Data moves between devices by JAX's collectives and lax.ppermute only.
A program may use at most 64 MiB of HBM per device.

```python
import math
import jax
import jax.numpy as jnp
import numpy as np
from jax import lax

NB = 1024
RMAX = 48
RMIN = 16
MTB = 1
MT = 32
TRD = 4
SB = 32
N_PROW = 8
N_PCOL = 32


def draw_points(key, part):
    total_bits = max(1, (MT - 1).bit_length())
    x_bits = (total_bits + 1) // 2
    y_bits = total_bits // 2
    blocks = jnp.arange(MT, dtype=jnp.int32)
    cell_x = jnp.zeros((MT,), jnp.float32)
    cell_y = jnp.zeros((MT,), jnp.float32)
    for level in range(total_bits):
        digit = (blocks // 2 ** level % 2).astype(jnp.float32)
        if level % 2 == 0:
            cell_x = cell_x + digit * float(2 ** (level // 2))
        else:
            cell_y = cell_y + digit * float(2 ** (level // 2))
    key_jitter = jax.random.fold_in(key, 11)
    key_spread = jax.random.fold_in(key, 23)
    key_select = jax.random.fold_in(key, 37)
    jitter = jax.random.uniform(key_jitter, (MT, 2, NB), jnp.float32)
    spread = jax.random.uniform(key_spread, (MT, 2, NB), jnp.float32)
    select = jax.random.uniform(key_select, (MT, 1, NB), jnp.float32)
    share = 0.25
    coord_x = (cell_x[:, None] + jitter[:, 0]) / float(2 ** x_bits)
    coord_y = (cell_y[:, None] + jitter[:, 1]) / float(2 ** y_bits)
    local = jnp.stack([coord_x, coord_y], axis=1)
    placed = jnp.where(select < share, spread, local)
    return placed.reshape(MTB, N_PCOL, 2, NB)


def plant(drawn, key, low, largest):
    longest = drawn.shape.index(max(drawn.shape))
    spots = []
    for shift in (0, 1):
        where = [jax.random.randint(jax.random.fold_in(key, axis), (), 0, length) for axis, length in enumerate(drawn.shape)]
        where[longest] = (where[longest] + shift) % drawn.shape[longest]
        spots.append(tuple(where))
    return drawn.at[spots[0]].set(low).at[spots[1]].set(largest)


def block_levels(stream_key, extent, shards, least, high):
    def one(axis_at, parts):
        heights = jax.random.uniform(jax.random.fold_in(jax.random.fold_in(stream_key, 6), axis_at), (parts,), jnp.float32, least / len(shards), high / len(shards))
        return jnp.repeat(jnp.exp(heights), extent[axis_at] // parts).reshape((-1,) + (1,) * (len(extent) - axis_at - 1))

    gain = one(*shards[0])
    for cut in shards[1:]:
        gain = gain * one(*cut)
    return gain


def noise(rng, shape, scale, reach, cuts=(), held_as=jnp.bfloat16):
    entries = scale * jax.random.normal(rng, shape, jnp.float32)
    if cuts:
        entries = entries * block_levels(rng, shape, cuts, -0.22, 0.18)
    return jnp.clip(entries, -reach, reach).astype(held_as)


def setup_inputs(seed: int = 0) -> dict:
    key_list = jax.random.split(jax.random.key(seed), 7)
    points = draw_points(jax.random.fold_in(key_list[6], 71), 0)
    range_length = jnp.clip(jnp.exp(jax.random.uniform(key_list[1], (1,), jnp.float32, math.log(0.05), math.log(0.15))), 0.05, 0.15)
    smoothness = jax.random.randint(key_list[2], (1,), 0, 3).astype(jnp.int32)
    sketch_bank = noise(key_list[3], (SB, RMAX, NB), 1.0, 6.0, ((0, 32),))
    sketch_ids = plant(jax.random.randint(key_list[4], (TRD, N_PROW, MTB, N_PCOL), 0, SB), jax.random.fold_in(key_list[4], 1), 0, SB - 1).astype(jnp.int32)
    tile_ranks = plant(jax.random.randint(key_list[5], (TRD, N_PROW, MTB, N_PCOL), RMIN, RMAX + 1), jax.random.fold_in(key_list[5], 1), RMIN, RMAX).astype(jnp.int32)
    return dict(points=points, range_length=range_length, smoothness=smoothness, sketch_bank=sketch_bank, sketch_ids=sketch_ids, tile_ranks=tile_ranks)


def kernel_factors(smoothness, range_length):
    morton_value = smoothness[0].astype(jnp.float32)
    kernel_scale = jnp.sqrt(2.0 * morton_value + 1.0) / range_length[0]
    linear_factor = jnp.where(smoothness[0] >= 1, 1.0, 0.0).astype(jnp.float32)
    squared_distance = jnp.where(smoothness[0] >= 2, 1.0 / 3.0, 0.0).astype(jnp.float32)
    return (kernel_scale, linear_factor, squared_distance)

def covariance_tile(row_locations, column_locations, kernel_scale, linear_factor, squared_distance):
    offset_horizontal = row_locations[0][:, None] - column_locations[0][None, :]
    offset_vertical = row_locations[1][:, None] - column_locations[1][None, :]
    scaled_distance = kernel_scale * jnp.sqrt(offset_horizontal * offset_horizontal + offset_vertical * offset_vertical)
    return (1.0 + linear_factor * scaled_distance + squared_distance * scaled_distance * scaled_distance) * jnp.exp(-scaled_distance)

def compress(tile_low, sketch, rank):
    keep = jnp.arange(sketch.shape[0]) < rank
    sketch = jnp.where(keep[:, None], sketch, jnp.zeros_like(sketch))
    sketched = lax.dot_general(sketch.astype(jnp.float32), tile_low.astype(jnp.float32), (((1,), (1,)), ((), ())), preferred_element_type=jnp.float32)
    product = jnp.dot(sketched.astype(jnp.bfloat16).astype(jnp.float32), tile_low.astype(jnp.float32), preferred_element_type=jnp.float32)
    gram = jnp.dot(sketched, sketched.T, precision=lax.Precision.HIGHEST)
    shift = 0.1 * jnp.trace(gram) / rank.astype(jnp.float32)
    gram = gram + jnp.diag(jnp.where(keep, shift, jnp.ones_like(shift)))
    factor = jnp.linalg.cholesky(gram)
    coeffs = jax.scipy.linalg.cho_solve((factor, True), product)
    approx = lax.dot_general(sketched, coeffs, (((0,), (0,)), ((), ())), precision=lax.Precision.HIGHEST)
    error = tile_low.astype(jnp.float32) - approx
    return (sketched, coeffs, jnp.sum(error * error))

def reference(points, range_length, smoothness, sketch_bank, sketch_ids, tile_ranks):
    every_block = points.reshape(MT, 2, NB)
    kernel_scale, linear_factor, squared_distance = kernel_factors(smoothness, range_length)
    pairs = np.array([(row, col) for row in range(MT) for col in range(row + 1)], np.int32)
    row_index = jnp.asarray(pairs[:, 0]).astype(jnp.int32)
    col_index = jnp.asarray(pairs[:, 1]).astype(jnp.int32)
    row_major = row_index // N_PROW
    row_minor = row_index % N_PROW
    col_major = col_index // N_PCOL
    col_minor = col_index % N_PCOL
    chosen_ids = sketch_ids[row_major, row_minor, col_major, col_minor]
    chosen_ranks = tile_ranks[row_major, row_minor, col_major, col_minor]

    def one_tile(inputs):
        row_number, column_number, sketch_id, rank = inputs
        tile_block = covariance_tile(every_block[row_number], every_block[column_number], kernel_scale, linear_factor, squared_distance)
        norm_sq = jnp.sum(tile_block * tile_block)
        tile_low = tile_block.astype(jnp.bfloat16)
        sketched, coeffs, err_sq = compress(tile_low, sketch_bank[sketch_id], rank)
        return (sketched, coeffs, norm_sq, err_sq)
    sketched_all, coeffs_all, norm_all, err_all = lax.map(one_tile, (row_index, col_index, chosen_ids, chosen_ranks))
    offdiag = row_index > col_index
    total = jnp.sum(jnp.where(offdiag, 2.0, 1.0) * norm_all)
    errors = jnp.where(offdiag, jnp.sqrt(err_all), jnp.sqrt(norm_all)) * MT / jnp.sqrt(total)
    shape_out = (TRD, N_PROW, MTB, N_PCOL, RMAX, NB)
    y_out = jnp.zeros(shape_out, jnp.float32).at[row_major, row_minor, col_major, col_minor].set(jnp.where(offdiag[:, None, None], sketched_all, 0.0))
    c_out = jnp.zeros(shape_out, jnp.float32).at[row_major, row_minor, col_major, col_minor].set(jnp.where(offdiag[:, None, None], coeffs_all, 0.0))
    err_out = jnp.zeros((TRD, N_PROW, MTB, N_PCOL), jnp.float32).at[row_major, row_minor, col_major, col_minor].set(errors)
    rank_out = jnp.sum(jnp.where(offdiag, chosen_ranks, 0)).astype(jnp.int32).reshape(1)
    return (y_out, c_out, err_out, rank_out)
```

```python
import functools

import jax
import jax.numpy as jnp
from jax import lax
from jax.experimental import pallas as pl
from jax.experimental.pallas import tpu as pltpu
from jax.sharding import Mesh
from jax.sharding import PartitionSpec as P

PCOL = ("pcol_0", "pcol_1", "pcol_2")
ALL = ("prow", "pcol_0", "pcol_1", "pcol_2")

TILE = 1024
RANKS = 48
SLOTS = 4
LOG2E = 1.4426950408889634
VMEM = pltpu.VMEM
SMEM = pltpu.SMEM


def spec(space):
    return pl.BlockSpec(memory_space=space)


def device_at(z, y, x, c):
    return ((z * 4 + y) * 4 + x) * 2 + c


def fetch_row_points(own):
    received = []
    for k in range(SLOTS):
        pairs = []
        for z in range(8):
            for y in range(4):
                for x in range(4):
                    for c in range(2):
                        source = device_at(2 * x + c, (y + k) % 4, z // 2, z % 2)
                        pairs.append((source, device_at(z, y, x, c)))
        received.append(lax.ppermute(own, ALL, pairs))
    return received


def plane_shift(value, shift, stage):
    pairs = []
    for y in range(4):
        for x in range(4):
            for c in range(2):
                if (c == 0) == (stage == 0):
                    to = (y, (x + shift) % 4, c)
                else:
                    to = ((y + shift) % 4, x, c)
                pairs.append(((y * 4 + x) * 2 + c, (to[0] * 4 + to[1]) * 2 + to[2]))
    return lax.ppermute(value, PCOL, pairs)


def swap_cores(value):
    return lax.ppermute(value, "pcol_2", [(0, 1), (1, 0)])


def sum_shifts(value, axis, shifts):
    size = {"prow": 8, "pcol_0": 4, "pcol_1": 4, "pcol_2": 2}[axis]
    moved = [
        lax.ppermute(value, axis, [(i, (i + s) % size) for i in range(size)]) for s in shifts
    ]
    for part in moved:
        value = value + part
    return value


def sum_pairs(value, axis, bit):
    size = {"prow": 8, "pcol_0": 4, "pcol_1": 4, "pcol_2": 2}[axis]
    return value + lax.ppermute(value, axis, [(i, i ^ bit) for i in range(size)])


def covariance_kernel(place, factors, ranks, rows, cols, low, norms, share, turned, xb, yb):
    p, q, y = place[0], place[1], place[2]
    scale = factors[0]
    linear = factors[1] * scale
    square = factors[2] * scale * scale
    power = scale * (-LOG2E)
    share[...] = jnp.zeros_like(share)

    def slot(k, rank_sum):
        a = (y + k) & 3
        i = a * 8 + p
        norms[k] = jnp.zeros((8, 128), jnp.float32)

        @pl.when(q <= i)
        def _():
            points = rows[k]
            for g in range(8):
                turned[pl.ds(2 * g, 2), :] = points[:, g * 128 : (g + 1) * 128]
            columns = jnp.transpose(turned[...])
            for g in range(8):
                xb[pl.ds(g * 128, 128), :] = jnp.broadcast_to(
                    columns[:, 2 * g : 2 * g + 1], (128, 128)
                )
                yb[pl.ds(g * 128, 128), :] = jnp.broadcast_to(
                    columns[:, 2 * g + 1 : 2 * g + 2], (128, 128)
                )

            def strip(s, acc):
                at = pl.ds(pl.multiple_of(s * 16, 16), 16)
                xr = xb[at, :]
                yr = yb[at, :]
                for n in range(8):
                    lanes = slice(n * 128, (n + 1) * 128)
                    dx = xr - cols[0:1, lanes]
                    dy = yr - cols[1:2, lanes]
                    d2 = dx * dx + dy * dy
                    r = d2 * lax.rsqrt(jnp.maximum(d2, 1e-30))
                    v = (1.0 + r * (linear + square * r)) * jnp.exp2(power * r)
                    low[k, at, lanes] = v.astype(jnp.bfloat16)
                    v2 = v * v
                    acc = acc + (v2[0:8] + v2[8:16])
                return acc

            acc = lax.fori_loop(0, 64, strip, jnp.zeros((8, 128), jnp.float32), unroll=2)
            norms[k] = acc
            share[0:8, :] += jnp.where(q < i, 2.0, 1.0) * acc

        return rank_sum + jnp.where(q < i, ranks[a], 0)

    rank_sum = lax.fori_loop(0, SLOTS, slot, jnp.int32(0))
    first = (lax.broadcasted_iota(jnp.int32, (8, 128), 0) == 0) & (
        lax.broadcasted_iota(jnp.int32, (8, 128), 1) == 0
    )
    share[8:16, :] = jnp.where(first, rank_sum.astype(jnp.float32), 0.0)


def select_kernel(place, mine_ids, their_ids, s0, s1, s2, s3, mine, theirs, sems):
    y, x, c = place[2], place[3], place[4]
    u = jnp.where(c == 0, x, y)
    v = jnp.where(c == 0, y, x)
    held = (s0, s1, s2, s3)

    def each(act):
        for w in range(2 * SLOTS):
            k = w % SLOTS
            ids = mine_ids if w < SLOTS else their_ids
            out = mine if w < SLOTS else theirs
            e = ids[k]
            ye, xe, ce = e // 8, (e // 2) & 3, e & 1
            ue = jnp.where(c == 0, xe, ye)
            ve = jnp.where(c == 0, ye, xe)
            inner = (u - ue) & 3
            outer = (v - ve) & 3
            for o in range(4):

                @pl.when((ce == c) & (outer == o))
                def _(o=o, k=k, w=w, out=out, inner=inner):
                    act(pltpu.make_async_copy(held[o].at[inner], out.at[k], sems.at[w]))

    each(lambda copy: copy.start())
    each(lambda copy: copy.wait())


def split3(value):
    high = value.astype(jnp.bfloat16)
    rest = value - high.astype(jnp.float32)
    mid = rest.astype(jnp.bfloat16)
    return high, mid, (rest - mid.astype(jnp.float32)).astype(jnp.bfloat16)


def dot_nt(a, b, **kw):
    return lax.dot_general(
        a, b, (((1,), (1,)), ((), ())), preferred_element_type=jnp.float32, **kw
    )


def sketch_kernel(place, ids, ranks, low, mine, got, y_out, w_out, h_out):
    p, q, y, c = place[0], place[1], place[2], place[4]

    def slot(k, carry):
        a = (y + k) & 3
        active = q < a * 8 + p

        @pl.when(jnp.logical_not(active))
        def _():
            y_out[a] = jnp.zeros((RANKS, TILE), jnp.float32)

        @pl.when(active)
        def _():
            rank = ranks[a]
            own = (ids[a] & 1) == c
            sketch = jnp.where(own, mine[a].astype(jnp.float32), got[a].astype(jnp.float32))
            row = lax.broadcasted_iota(jnp.int32, (RANKS, TILE), 0)
            sketch = jnp.where(row < rank, sketch, 0.0).astype(jnp.bfloat16)
            tile = low[k]
            sketched = dot_nt(sketch, tile)
            y_out[a] = sketched
            w_out[a] = jnp.dot(
                sketched.astype(jnp.bfloat16), tile, preferred_element_type=jnp.float32
            )
            high, mid, rest = split3(sketched)
            one = dot_nt(jnp.concatenate([high, mid, rest], 0), high)
            two = dot_nt(jnp.concatenate([high, mid], 0), mid)
            three = dot_nt(high, rest)
            gram = (
                one[0:48] + (one[48:96] + two[0:48]) + (one[96:144] + two[48:96] + three)
            )
            r2 = lax.broadcasted_iota(jnp.int32, (RANKS, RANKS), 0)
            c2 = lax.broadcasted_iota(jnp.int32, (RANKS, RANKS), 1)
            diag = r2 == c2
            trace = jnp.sum(jnp.where(diag, gram, 0.0))
            mu = 0.1 * trace / rank.astype(jnp.float32)
            h_out[a] = gram + jnp.where(diag, jnp.where(r2 < rank, mu, 1.0), 0.0)

        return carry

    lax.fori_loop(0, SLOTS, slot, 0)


def inverse_kernel(h_in, out, *, panel):
    count = SLOTS
    lane = lax.broadcasted_iota(jnp.int32, (1, RANKS), 1)
    sub = lax.broadcasted_iota(jnp.int32, (RANKS, 1), 0)
    mats = [h_in[t] for t in range(count)]
    for start in range(0, RANKS, panel):
        cols = [
            [
                jnp.broadcast_to(m[:, start + j : start + j + 1], (RANKS, RANKS))
                for j in range(panel)
            ]
            for m in mats
        ]
        for j in range(panel):
            k = start + j
            for t in range(count):
                a = mats[t]
                col = cols[t][j]
                d = 1.0 / col[k : k + 1, :]
                row = jnp.where(lane == k, d, a[k : k + 1, :] * d)
                for later in range(j + 1, panel):
                    factor = cols[t][later][k : k + 1, :] * d
                    cols[t][later] = jnp.where(
                        sub == k, factor, cols[t][later] - col * factor
                    )
                mats[t] = jnp.where(sub == k, row, jnp.where(lane == k, 0.0, a) - col * row)
    for t in range(count):
        out[t] = mats[t]


def coefficient_kernel(place, low, y_in, w_in, h_inv, c_out, err_out, yz, cz):
    p, q, y = place[0], place[1], place[2]

    def slot(k, carry):
        a = (y + k) & 3
        active = q < a * 8 + p
        err_out[k] = jnp.zeros((8, 128), jnp.float32)

        @pl.when(jnp.logical_not(active))
        def _():
            c_out[a] = jnp.zeros((RANKS, TILE), jnp.float32)

        @pl.when(active)
        def _():
            ih, im, il = split3(h_inv[a])
            wh, wm, wl = split3(w_in[a])
            dot = functools.partial(jnp.dot, preferred_element_type=jnp.float32)
            one = dot(jnp.concatenate([ih, im, il], 0), wh)
            two = dot(jnp.concatenate([ih, im], 0), wm)
            three = dot(ih, wl)
            coeffs = (
                one[0:48] + (one[48:96] + two[0:48]) + (one[96:144] + two[48:96] + three)
            )
            c_out[a] = coeffs
            ch, cm, _unused = split3(coeffs)
            yh, ym, _unused = split3(y_in[a])
            yz[...] = jnp.concatenate([yh, yh, ym], 0)
            cz[...] = jnp.concatenate([ch, cm, ch], 0)

            acc = jnp.zeros((8, 128), jnp.float32)
            for s in range(8):
                lhs = yz[:, s * 128 : (s + 1) * 128]
                for n in range(2):
                    approx = lax.dot_general(
                        lhs,
                        cz[:, n * 512 : (n + 1) * 512],
                        (((0,), (0,)), ((), ())),
                        preferred_element_type=jnp.float32,
                    )
                    rest = (
                        low[k, s * 128 : (s + 1) * 128, n * 512 : (n + 1) * 512].astype(
                            jnp.float32
                        )
                        - approx
                    )
                    rest = rest * rest
                    acc = acc + jnp.sum(rest.reshape(16, 8, 4, 128), axis=(0, 2))
            err_out[k] = acc

        return carry

    lax.fori_loop(0, SLOTS, slot, 0)


def error_kernel(place, total, norms, errs, out, rank_out):
    p, q, y = place[0], place[1], place[2]
    whole = jnp.sum(total[0:8, :])
    row = lax.broadcasted_iota(jnp.int32, (SLOTS, 128), 0)
    values = jnp.zeros((SLOTS, 128), jnp.float32)
    for k in range(SLOTS):
        a = (y + k) & 3
        i = a * 8 + p
        kept = jnp.where(q < i, jnp.sum(errs[k]), jnp.where(q == i, jnp.sum(norms[k]), 0.0))
        values = jnp.where(row == a, kept, values)
    out[...] = 32.0 * jnp.sqrt(values) / jnp.sqrt(jnp.full((SLOTS, 128), whole, jnp.float32))
    rank_out[0] = jnp.sum(total[8:16, :]).astype(jnp.int32)


def per_device(points, range_length, smoothness, sketch_bank, sketch_ids, tile_ranks):
    f32, bf16, i32 = jnp.float32, jnp.bfloat16, jnp.int32
    shape = jax.ShapeDtypeStruct
    p = lax.axis_index("prow")
    y, x, c = (lax.axis_index(n) for n in PCOL)
    place = jnp.stack([p, (y * 4 + x) * 2 + c, y, x, c]).astype(i32)
    s = smoothness[0]
    factors = jnp.stack(
        [
            jnp.sqrt(2.0 * s.astype(f32) + 1.0) / range_length[0],
            jnp.where(s >= 1, 1.0, 0.0).astype(f32),
            jnp.where(s >= 2, 1.0 / 3.0, 0.0).astype(f32),
        ]
    )
    ids = sketch_ids.reshape(SLOTS)
    ranks = tile_ranks.reshape(SLOTS)
    own = points.reshape(2, TILE)

    first = [sketch_bank] + [plane_shift(sketch_bank, sh, 0) for sh in (1, 2, 3)]
    rows = jnp.stack(fetch_row_points(own))
    their_ids = swap_cores(ids)
    group = jnp.concatenate(first, 0)
    held = [group] + [plane_shift(group, sh, 1) for sh in (1, 2, 3)]

    low, norms, share = pl.pallas_call(
        covariance_kernel,
        out_shape=(
            shape((SLOTS, TILE, TILE), bf16),
            shape((SLOTS, 8, 128), f32),
            shape((16, 128), f32),
        ),
        in_specs=[spec(SMEM)] * 3 + [spec(VMEM)] * 2,
        out_specs=[spec(VMEM)] * 3,
        scratch_shapes=[
            VMEM((128, 128), f32),
            VMEM((TILE, 128), f32),
            VMEM((TILE, 128), f32),
        ],
        compiler_params=pltpu.CompilerParams(vmem_limit_bytes=16 << 20),
        cost_estimate=pl.CostEstimate(
            flops=10_000_000_0, bytes_accessed=8 << 20, transcendentals=8 << 20
        ),
        name="covariance",
    )(place, factors, ranks, rows, own)

    total = sum_pairs(share, "pcol_2", 1)
    total = sum_shifts(total, "pcol_1", (1, 2, 3))
    total = sum_shifts(total, "pcol_0", (1, 2, 3))
    total = sum_pairs(total, "prow", 1)
    total = sum_shifts(total, "prow", (2, 4, 6))

    mine, theirs = pl.pallas_call(
        select_kernel,
        out_shape=(shape((SLOTS, RANKS, TILE), bf16),) * 2,
        in_specs=[spec(SMEM)] * 3 + [spec(pl.ANY)] * 4,
        out_specs=[spec(VMEM)] * 2,
        scratch_shapes=[pltpu.SemaphoreType.DMA((2 * SLOTS,))],
        name="select",
    )(place, ids, their_ids, *held)
    got = swap_cores(theirs)

    y_all, w_all, h_all = pl.pallas_call(
        sketch_kernel,
        out_shape=(
            shape((SLOTS, RANKS, TILE), f32),
            shape((SLOTS, RANKS, TILE), f32),
            shape((SLOTS, RANKS, RANKS), f32),
        ),
        in_specs=[spec(SMEM)] * 3 + [spec(VMEM)] * 3,
        out_specs=[spec(VMEM)] * 3,
        compiler_params=pltpu.CompilerParams(vmem_limit_bytes=24 << 20),
        cost_estimate=pl.CostEstimate(
            flops=1_000_000_000, bytes_accessed=8 << 20, transcendentals=0
        ),
        name="sketch",
    )(place, ids, ranks, low, mine, got)

    h_inv = pl.pallas_call(
        functools.partial(inverse_kernel, panel=4),
        out_shape=shape((SLOTS, RANKS, RANKS), f32),
        in_specs=[spec(VMEM)],
        out_specs=spec(VMEM),
        cost_estimate=pl.CostEstimate(
            flops=100_000_000, bytes_accessed=1 << 16, transcendentals=0
        ),
        name="inverse",
    )(h_all)

    c_all, errs = pl.pallas_call(
        coefficient_kernel,
        out_shape=(shape((SLOTS, RANKS, TILE), f32), shape((SLOTS, 8, 128), f32)),
        in_specs=[spec(SMEM)] + [spec(VMEM)] * 4,
        out_specs=[spec(VMEM)] * 2,
        scratch_shapes=[VMEM((3 * RANKS, TILE), bf16)] * 2,
        compiler_params=pltpu.CompilerParams(vmem_limit_bytes=24 << 20),
        cost_estimate=pl.CostEstimate(
            flops=1_000_000_000, bytes_accessed=8 << 20, transcendentals=0
        ),
        name="coefficients",
    )(place, low, y_all, w_all, h_inv)

    errors, rank_out = pl.pallas_call(
        error_kernel,
        out_shape=(shape((SLOTS, 128), f32), shape((1,), i32)),
        in_specs=[spec(SMEM)] + [spec(VMEM)] * 3,
        out_specs=[spec(VMEM), spec(SMEM)],
        name="errors",
    )(place, total, norms, errs)

    wide = (SLOTS, 1, 1, 1, RANKS, TILE)
    return (
        y_all.reshape(wide),
        c_all.reshape(wide),
        errors[:, 0].reshape(SLOTS, 1, 1, 1),
        rank_out,
    )


def solution(mesh):
    split = Mesh(
        mesh.devices.reshape(mesh.shape["prow"], 4, 4, 2), ("prow", "pcol_0", "pcol_1", "pcol_2")
    )
    placed = (
        P(None, PCOL, None, None),
        P(),
        P(),
        P(PCOL, None, None),
        P(None, "prow", None, PCOL),
        P(None, "prow", None, PCOL),
    )
    return jax.shard_map(
        per_device,
        mesh=split,
        in_specs=placed,
        out_specs=(
            P(None, "prow", None, PCOL, None, None),
            P(None, "prow", None, PCOL, None, None),
            P(None, "prow", None, PCOL),
            P(),
        ),
        check_vma=False,
    )
```

```python
import functools

import jax
import jax.numpy as jnp
from jax import lax
from jax.experimental import pallas as pl
from jax.experimental.pallas import tpu as pltpu
from jax.sharding import Mesh
from jax.sharding import PartitionSpec as P


PCOL = ("pcol_0", "pcol_1", "pcol_2")

TILE = 1024
RANKS = 48
SLOTS = 4
LOG2E = 1.4426950408889634
VMEM = pltpu.VMEM
SMEM = pltpu.SMEM


def spec(space):
    return pl.BlockSpec(memory_space=space)


def to_all(value, axes):
    copies = jnp.broadcast_to(value, (lax.axis_size(axes), *value.shape))
    return lax.all_to_all(copies, axes, split_axis=0, concat_axis=0)


def swap_cores(value):
    return lax.ppermute(value, "pcol_2", [(0, 1), (1, 0)])


def add_kernel(*refs):
    total = refs[0][...]
    for part in refs[1:-1]:
        total = total + part[...]
    refs[-1][...] = jnp.broadcast_to(total, refs[-1].shape)


def add_up(parts, out_shape):
    return pl.pallas_call(
        add_kernel,
        out_shape=jax.ShapeDtypeStruct(out_shape, jnp.float32),
        in_specs=[spec(VMEM)] * len(parts),
        out_specs=spec(VMEM),
        compiler_params=pltpu.CompilerParams(vmem_limit_bytes=1 << 20),
    )(*parts)


def from_others(value, axis):
    size = {"prow": 8, "pcol_0": 4, "pcol_1": 4, "pcol_2": 2}[axis]
    return [value] + [
        lax.ppermute(value, axis, [(i, (i + s) % size) for i in range(size)])
        for s in range(1, size)
    ]


def covariance_kernel(place, order, factors, ranks, rows, cols, low_hbm, norms, share, low, turned, xb, yb, sems):
    p, q = place[0], place[1]
    scale = factors[0]
    square = factors[1] * scale * scale
    power = scale * (-LOG2E)

    def tile(k, poly):
        points = rows[k * 8 + p]
        for g in range(8):
            turned[pl.ds(2 * g, 2), :] = points[:, g * 128 : (g + 1) * 128]
        columns = jnp.transpose(turned[...])
        for g in range(8):
            at = pl.ds(g * 128, 128)
            xb[at, :] = jnp.broadcast_to(columns[:, 2 * g : 2 * g + 1], (128, 128))
            yb[at, :] = jnp.broadcast_to(columns[:, 2 * g + 1 : 2 * g + 2], (128, 128))

        def strip(s, acc):
            at = pl.ds(pl.multiple_of(s * 16, 16), 16)
            xr = xb[at, :]
            yr = yb[at, :]
            for n in range(8):
                lanes = slice(n * 128, (n + 1) * 128)
                dx = xr - cols[0:1, lanes]
                dy = yr - cols[1:2, lanes]
                d2 = dx * dx + dy * dy
                r = d2 * lax.rsqrt(jnp.maximum(d2, 1e-30))
                v = poly(r, jnp.exp2(power * r))
                low[k, at, lanes] = v.astype(jnp.bfloat16)
                v2 = v * v
                acc = acc + (v2[0:8] + v2[8:16])
            return acc

        norms[k] = lax.fori_loop(0, 64, strip, jnp.zeros((8, 128), jnp.float32), unroll=2)

    polys = (
        lambda r, e: e,
        lambda r, e: (1.0 + scale * r) * e,
        lambda r, e: (1.0 + r * (scale + square * r)) * e,
    )

    def slot(k, carry):
        rank_sum, acc = carry
        i = k * 8 + p
        norms[k] = jnp.zeros((8, 128), jnp.float32)
        for which in range(3):

            @pl.when((q <= i) & (order[0] == which))
            def _(which=which):
                tile(k, polys[which])

        @pl.when(q <= i)
        def _():
            pltpu.make_async_copy(low.at[k], low_hbm.at[k], sems.at[k]).start()

        acc = acc + jnp.where(q < i, 2.0, 1.0) * norms[k]
        return rank_sum + jnp.where(q < i, ranks[k], 0), acc

    rank_sum, acc = lax.fori_loop(
        0, SLOTS, slot, (jnp.int32(0), jnp.zeros((8, 128), jnp.float32))
    )
    for k in range(SLOTS):

        @pl.when(q <= k * 8 + p)
        def _(k=k):
            pltpu.make_async_copy(low.at[k], low_hbm.at[k], sems.at[k]).wait()

    acc = jnp.sum(acc, axis=0, keepdims=True)
    lane = lax.broadcasted_iota(jnp.int32, (1, 128), 1)
    both = jnp.concatenate([acc, jnp.where(lane == 0, rank_sum.astype(jnp.float32), 0.0)], 0)
    share[...] = both[None]


def select_kernel(place, their_ids, held, theirs, sems):
    c = place[2]

    def each(act):
        for k in range(SLOTS):
            e = their_ids[k]

            @pl.when((e & 1) == c)
            def _(k=k, e=e):
                act(pltpu.make_async_copy(held.at[e // 2], theirs.at[k], sems.at[k]))

    each(lambda copy: copy.start())
    each(lambda copy: copy.wait())


def split3(value):
    high = value.astype(jnp.bfloat16)
    rest = value - high.astype(jnp.float32)
    mid = rest.astype(jnp.bfloat16)
    return high, mid, (rest - mid.astype(jnp.float32)).astype(jnp.bfloat16)


def dot_nt(a, b, **kw):
    return lax.dot_general(
        a, b, (((1,), (1,)), ((), ())), preferred_element_type=jnp.float32, **kw
    )


def three_pass(parts_a, parts_b, dot):
    n = RANKS
    one = dot(jnp.concatenate(parts_a, 0), parts_b[0])
    two = dot(jnp.concatenate(parts_a[:2], 0), parts_b[1])
    three = dot(parts_a[0], parts_b[2])
    return one[0:n] + (one[n : 2 * n] + two[0:n]) + (one[2 * n :] + two[n:] + three)


HALF = 64


def inverses(pairs, panel):
    whole = (RANKS, 2 * HALF)
    lane = lax.broadcasted_iota(jnp.int32, (1, 2 * HALF), 1)
    column = lane & (HALF - 1)
    side = lax.broadcasted_iota(jnp.int32, whole, 1) & HALF
    sub = lax.broadcasted_iota(jnp.int32, (RANKS, 1), 0)
    pairs = list(pairs)
    for start in range(0, RANKS, panel):
        cols = [
            [
                jnp.take_along_axis(m, side + (start + j), axis=1, mode="promise_in_bounds")
                for j in range(panel)
            ]
            for m in pairs
        ]
        for j in range(panel):
            k = start + j
            for t in range(len(pairs)):
                a = pairs[t]
                col = cols[t][j]
                d = 1.0 / col[k : k + 1, :]
                row = jnp.where(column == k, d, a[k : k + 1, :] * d)
                for later in range(j + 1, panel):
                    factor = cols[t][later][k : k + 1, :] * d
                    cols[t][later] = jnp.where(
                        sub == k, factor, cols[t][later] - col * factor
                    )
                pairs[t] = jnp.where(
                    sub == k, row, jnp.where(column == k, 0.0, a) - col * row
                )
    return pairs


def compress_kernel(
    place, ids, ranks, low_hbm, held, got, y_out, c_out, err_out,
    low, sk, w_all, h_all, zt, cz, sems, low_sems,
):
    p, q, c = place[0], place[1], place[2]
    dot = functools.partial(jnp.dot, preferred_element_type=jnp.float32)

    def slot_of(k):
        return k, q < k * 8 + p

    def each(act):
        for k in range(SLOTS):
            a, active = slot_of(k)
            e = ids[a]

            @pl.when(active & ((e & 1) == c))
            def _(k=k, e=e):
                act(pltpu.make_async_copy(held.at[e // 2], sk.at[k], sems.at[k]))

            @pl.when(active & ((e & 1) != c))
            def _(k=k, a=a):
                act(pltpu.make_async_copy(got.at[a], sk.at[k], sems.at[k]))

    each(lambda copy: copy.start())
    loads = [
        pltpu.make_async_copy(low_hbm.at[k], low.at[k], low_sems.at[k]) for k in range(SLOTS)
    ]
    for k in range(SLOTS):
        pl.when(slot_of(k)[1])(loads[k].start)
    r2 = lax.broadcasted_iota(jnp.int32, (RANKS, RANKS), 0)
    c2 = lax.broadcasted_iota(jnp.int32, (RANKS, RANKS), 1)
    diag = r2 == c2
    for k in range(SLOTS):
        a, active = slot_of(k)

        @pl.when(jnp.logical_not(active))
        def _():
            y_out[a] = jnp.zeros((RANKS, TILE), jnp.float32)
            c_out[a] = jnp.zeros((RANKS, TILE), jnp.float32)
            h_all[k // 2, :, pl.ds(HALF * (k % 2), RANKS)] = jnp.where(diag, 1.0, 0.0)

    each(lambda copy: copy.wait())

    for k in range(SLOTS):
        a, active = slot_of(k)

        @pl.when(active)
        def _(k=k, a=a):
            loads[k].wait()
            rank = ranks[a]
            row = lax.broadcasted_iota(jnp.int32, (RANKS, TILE), 0)
            chosen = jnp.where(row < rank, sk[k].astype(jnp.float32), 0.0).astype(jnp.bfloat16)
            sketched = jnp.transpose(dot_nt(low[k], chosen))
            y_out[a] = sketched
            parts = split3(sketched)
            w_all[k] = dot(parts[0], low[k])
            gram = three_pass(parts, parts, dot_nt)
            trace = jnp.sum(jnp.where(diag, gram, 0.0))
            mu = 0.1 * trace / rank.astype(jnp.float32)
            h_all[k // 2, :, pl.ds(HALF * (k % 2), RANKS)] = gram + jnp.where(
                diag, jnp.where(r2 < rank, mu, 1.0), 0.0
            )

    lanes = lax.broadcasted_iota(jnp.int32, (RANKS, 2 * HALF), 1)
    used = (lanes & (HALF - 1)) < RANKS
    pairs = [jnp.where(used, h_all[t], 0.0) for t in range(SLOTS // 2)]
    for t, inverse in enumerate(inverses(pairs, 4)):
        h_all[t] = inverse

    for k in range(SLOTS):
        a, active = slot_of(k)
        err_out[k] = jnp.zeros((8, 128), jnp.float32)

        @pl.when(active)
        def _(k=k, a=a):
            inverse = h_all[k // 2, :, pl.ds(HALF * (k % 2), RANKS)]
            coeffs = three_pass(split3(inverse), split3(w_all[k]), dot)
            c_out[a] = coeffs
            ch, cm, _unused = split3(coeffs)
            cz[...] = jnp.concatenate([ch, cm, ch], 0)
            yh, ym, _unused = split3(y_out[a])
            zt[...] = jnp.transpose(jnp.concatenate([yh, yh, ym], 0))
            acc = jnp.zeros((8, 128), jnp.float32)
            for n in range(4):
                lanes = slice(n * 256, (n + 1) * 256)
                approx = dot(zt[...], cz[:, lanes])
                rest = low[k, :, lanes].astype(jnp.float32) - approx
                rest = rest * rest
                rest = rest[:, :128] + rest[:, 128:]
                acc = acc + jnp.sum(rest.reshape(128, 8, 128), axis=0)
            err_out[k] = acc


def error_kernel(place, total, norms, errs, out, rank_out):
    p, q = place[0], place[1]
    summed = jnp.sum(total[...], axis=0)
    whole = jnp.sum(summed[0:1, :])
    lane = lax.broadcasted_iota(jnp.int32, (1, 128), 1)
    values = jnp.zeros((1, 128), jnp.float32)
    for k in range(SLOTS):
        i = k * 8 + p
        kept = jnp.where(q < i, jnp.sum(errs[k]), jnp.where(q == i, jnp.sum(norms[k]), 0.0))
        values = jnp.where(lane == k, kept, values)
    result = 32.0 * jnp.sqrt(values) / jnp.sqrt(jnp.full((1, 128), whole, jnp.float32))
    out[...] = result[:, :SLOTS]
    rank_out[0] = jnp.sum(summed[1:2, :]).astype(jnp.int32)


def device_program(points, range_length, smoothness, sketch_bank, sketch_ids, tile_ranks):
    f32, bf16, i32 = jnp.float32, jnp.bfloat16, jnp.int32
    shape = jax.ShapeDtypeStruct
    p = lax.axis_index("prow")
    y, x, c = (lax.axis_index(n) for n in PCOL)
    place = jnp.stack([p, (y * 4 + x) * 2 + c, c]).astype(i32)
    s = smoothness[0]
    factors = jnp.stack(
        [
            jnp.sqrt(2.0 * s.astype(f32) + 1.0) / range_length[0],
            jnp.float32(1.0 / 3.0),
        ]
    )
    ids = sketch_ids.reshape(SLOTS)
    ranks = tile_ranks.reshape(SLOTS)
    own = points.reshape(2, TILE)

    order = smoothness.astype(i32)
    rows = to_all(own, PCOL)
    held = to_all(sketch_bank[0], ("pcol_0", "pcol_1"))
    their_ids = swap_cores(ids)

    low, norms, share = pl.pallas_call(
        covariance_kernel,
        out_shape=(
            shape((SLOTS, TILE, TILE), bf16),
            shape((SLOTS, 8, 128), f32),
            shape((1, 2, 128), f32),
        ),
        in_specs=[spec(SMEM)] * 4 + [spec(VMEM)] * 2,
        out_specs=[spec(pltpu.HBM)] + [spec(VMEM)] * 2,
        scratch_shapes=[
            VMEM((SLOTS, TILE, TILE), bf16),
            VMEM((128, 128), f32),
            VMEM((TILE, 128), f32),
            VMEM((TILE, 128), f32),
            pltpu.SemaphoreType.DMA((SLOTS,)),
        ],
        compiler_params=pltpu.CompilerParams(vmem_limit_bytes=50 << 20),
        cost_estimate=pl.CostEstimate(
            flops=100_000_000, bytes_accessed=8 << 20, transcendentals=8 << 20
        ),
        name="covariance",
    )(place, order, factors, ranks, rows, own)

    small = (1, 2, 128)
    share = add_up(from_others(share, "pcol_2"), small)
    share = add_up(from_others(share, "pcol_1"), small)
    share = from_others(share, "pcol_0")
    again = add_up(share, (8, 2, 128))

    theirs = pl.pallas_call(
        select_kernel,
        out_shape=shape((SLOTS, RANKS, TILE), bf16),
        in_specs=[spec(SMEM)] * 2 + [spec(pl.ANY)],
        out_specs=spec(VMEM),
        scratch_shapes=[pltpu.SemaphoreType.DMA((SLOTS,))],
        compiler_params=pltpu.CompilerParams(vmem_limit_bytes=4 << 20),
        name="select",
    )(place, their_ids, held)
    got = swap_cores(theirs)
    total = lax.all_to_all(again, "prow", split_axis=0, concat_axis=0)

    y_all, c_all, errs = pl.pallas_call(
        compress_kernel,
        out_shape=(
            shape((SLOTS, RANKS, TILE), f32),
            shape((SLOTS, RANKS, TILE), f32),
            shape((SLOTS, 8, 128), f32),
        ),
        in_specs=[spec(SMEM)] * 3 + [spec(pltpu.HBM)] + [spec(pl.ANY)] * 2,
        out_specs=[spec(VMEM)] * 3,
        scratch_shapes=[
            VMEM((SLOTS, TILE, TILE), bf16),
            VMEM((SLOTS, RANKS, TILE), bf16),
            VMEM((SLOTS, RANKS, TILE), f32),
            VMEM((SLOTS // 2, RANKS, 2 * HALF), f32),
            VMEM((TILE, 3 * RANKS), bf16),
            VMEM((3 * RANKS, TILE), bf16),
            pltpu.SemaphoreType.DMA((SLOTS,)),
            pltpu.SemaphoreType.DMA((SLOTS,)),
        ],
        compiler_params=pltpu.CompilerParams(vmem_limit_bytes=60 << 20),
        cost_estimate=pl.CostEstimate(
            flops=2_000_000_000, bytes_accessed=8 << 20, transcendentals=0
        ),
        name="compress",
    )(place, ids, ranks, low, held, got)

    errors, rank_out = pl.pallas_call(
        error_kernel,
        out_shape=(shape((1, SLOTS), f32), shape((1,), i32)),
        in_specs=[spec(SMEM)] + [spec(VMEM)] * 3,
        out_specs=[spec(VMEM), spec(SMEM)],
        compiler_params=pltpu.CompilerParams(vmem_limit_bytes=4 << 20),
        name="errors",
    )(place, total, norms, errs)

    wide = (SLOTS, 1, 1, 1, RANKS, TILE)
    return (
        y_all.reshape(wide),
        c_all.reshape(wide),
        errors.reshape(SLOTS, 1, 1, 1),
        rank_out,
    )


def solution(mesh):
    split = Mesh(
        mesh.devices.reshape(mesh.shape["prow"], 4, 4, 2), ("prow", "pcol_0", "pcol_1", "pcol_2")
    )
    placed = (
        P(None, PCOL, None, None),
        P(),
        P(),
        P(PCOL, None, None),
        P(None, "prow", None, PCOL),
        P(None, "prow", None, PCOL),
    )
    return jax.shard_map(
        device_program,
        mesh=split,
        in_specs=placed,
        out_specs=(
            P(None, "prow", None, PCOL, None, None),
            P(None, "prow", None, PCOL, None, None),
            P(None, "prow", None, PCOL),
            P(),
        ),
        check_vma=False,
    )
```

```python
import functools

import jax
import jax.numpy as jnp
from jax import lax
from jax.experimental import pallas as pl
from jax.experimental.pallas import tpu as pltpu
from jax.sharding import Mesh
from jax.sharding import PartitionSpec as P


PCOL = ("pcol_0", "pcol_1", "pcol_2")
ALL = ("prow", "pcol_0", "pcol_1", "pcol_2")

TILE = 1024
RANKS = 48
SLOTS = 4
PARTS = 4
LOG2E = 1.4426950408889634
VMEM = pltpu.VMEM
SMEM = pltpu.SMEM


def spec(space):
    return pl.BlockSpec(memory_space=space)


def to_all(value, axes):
    copies = jnp.broadcast_to(value, (lax.axis_size(axes), *value.shape))
    return lax.all_to_all(copies, axes, split_axis=0, concat_axis=0)


def plane_shift(value, shift, stage):
    pairs = []
    for y in range(4):
        for x in range(4):
            for c in range(2):
                if (c == 0) == (stage == 0):
                    to = (y, (x + shift) % 4, c)
                else:
                    to = ((y + shift) % 4, x, c)
                pairs.append(((y * 4 + x) * 2 + c, (to[0] * 4 + to[1]) * 2 + to[2]))
    return lax.ppermute(value, PCOL, pairs)


def group_kernel(*refs):
    parts, out, sems = refs[:-2], refs[-2], refs[-1]
    moves = [pltpu.make_async_copy(part, out.at[i], sems.at[i]) for i, part in enumerate(parts)]
    for move in moves:
        move.start()
    for move in moves:
        move.wait()


def bank_of_plane(own):
    parts = [own] + [plane_shift(own, shift, 0) for shift in (1, 2, 3)]
    group = pl.pallas_call(
        group_kernel,
        out_shape=jax.ShapeDtypeStruct((4, *own.shape), own.dtype),
        in_specs=[spec(VMEM)] * 4,
        out_specs=spec(pltpu.HBM),
        scratch_shapes=[pltpu.SemaphoreType.DMA((4,))],
        compiler_params=pltpu.CompilerParams(vmem_limit_bytes=4 << 20),
        name="group_bank",
    )(*parts)
    return [group] + [plane_shift(group, shift, 1) for shift in (1, 2, 3)]


def fetch_entry(place, entry, wanted, held, out, sem, act):
    c, y, x = place[2], place[3], place[4]
    dy = (y - (entry >> 3)) & 3
    dx = (x - ((entry >> 1) & 3)) & 3
    inner = jnp.where(c == 0, dx, dy)
    outer = jnp.where(c == 0, dy, dx)
    for o in range(4):

        @pl.when(wanted & ((entry & 1) == c) & (outer == o))
        def _(o=o):
            act(pltpu.make_async_copy(held[o].at[inner], out, sem))


def swap_cores(value):
    return lax.ppermute(value, "pcol_2", [(0, 1), (1, 0)])


def covariance_kernel(place, order, factors, ranks, rows, cols, low_hbm, norms, share, low, turned, xb, yb, sems):
    p, q = place[0], place[1]
    scale = factors[0]
    square = factors[1] * scale * scale
    power = scale * (-LOG2E)

    def tile(k, poly):
        points = rows[k * 8 + p]
        for g in range(8):
            turned[pl.ds(2 * g, 2), :] = points[:, g * 128 : (g + 1) * 128]
        columns = jnp.transpose(turned[...])
        for g in range(8):
            at = pl.ds(g * 128, 128)
            xb[at, :] = jnp.broadcast_to(columns[:, 2 * g : 2 * g + 1], (128, 128))
            yb[at, :] = jnp.broadcast_to(columns[:, 2 * g + 1 : 2 * g + 2], (128, 128))

        def strip(s, acc):
            at = pl.ds(pl.multiple_of(s * 16, 16), 16)
            xr = xb[at, :]
            yr = yb[at, :]
            for n in range(8):
                lanes = slice(n * 128, (n + 1) * 128)
                dx = xr - cols[0:1, lanes]
                dy = yr - cols[1:2, lanes]
                d2 = dx * dx + dy * dy
                r = d2 * lax.rsqrt(jnp.maximum(d2, 1e-30))
                v = poly(r, jnp.exp2(power * r))
                low[k, at, lanes] = v.astype(jnp.bfloat16)
                v2 = v * v
                acc = acc + (v2[0:8] + v2[8:16])
            return acc

        norms[k] = lax.fori_loop(0, 64, strip, jnp.zeros((8, 128), jnp.float32), unroll=2)

    polys = (
        lambda r, e: e,
        lambda r, e: (1.0 + scale * r) * e,
        lambda r, e: (1.0 + r * (scale + square * r)) * e,
    )

    def slot(k, carry):
        rank_sum, acc = carry
        i = k * 8 + p
        norms[k] = jnp.zeros((8, 128), jnp.float32)
        for which in range(3):

            @pl.when((q <= i) & (order[0] == which))
            def _(which=which):
                tile(k, polys[which])

        @pl.when(q <= i)
        def _():
            pltpu.make_async_copy(low.at[k], low_hbm.at[k], sems.at[k]).start()

        acc = acc + jnp.where(q < i, 2.0, 1.0) * norms[k]
        return rank_sum + jnp.where(q < i, ranks[k], 0), acc

    rank_sum, acc = lax.fori_loop(
        0, SLOTS, slot, (jnp.int32(0), jnp.zeros((8, 128), jnp.float32))
    )
    for k in range(SLOTS):

        @pl.when(q <= k * 8 + p)
        def _(k=k):
            pltpu.make_async_copy(low.at[k], low_hbm.at[k], sems.at[k]).wait()

    acc = jnp.sum(acc, axis=0, keepdims=True)
    lane = lax.broadcasted_iota(jnp.int32, (1, 128), 1)
    both = jnp.concatenate([acc, jnp.where(lane == 0, rank_sum.astype(jnp.float32), 0.0)], 0)
    share[...] = both[None]


def select_kernel(place, their_ids, share, h0, h1, h2, h3, theirs, again, sems):
    def each(act):
        for k in range(SLOTS):
            fetch_entry(
                place, their_ids[k], True, (h0, h1, h2, h3), theirs.at[k], sems.at[k], act
            )

    each(lambda copy: copy.start())
    again[...] = jnp.broadcast_to(share[...], again.shape)
    each(lambda copy: copy.wait())


def split3(value):
    high = value.astype(jnp.bfloat16)
    rest = value - high.astype(jnp.float32)
    mid = rest.astype(jnp.bfloat16)
    return high, mid, (rest - mid.astype(jnp.float32)).astype(jnp.bfloat16)


def dot_nt(a, b, **kw):
    return lax.dot_general(
        a, b, (((1,), (1,)), ((), ())), preferred_element_type=jnp.float32, **kw
    )


def three_pass(parts_a, parts_b, dot):
    n = RANKS
    one = dot(jnp.concatenate(parts_a, 0), parts_b[0])
    two = dot(jnp.concatenate(parts_a[:2], 0), parts_b[1])
    three = dot(parts_a[0], parts_b[2])
    return one[0:n] + (one[n : 2 * n] + two[0:n]) + (one[2 * n :] + two[n:] + three)


HALF = 64


def inverses(pairs, panel):
    whole = (RANKS, 2 * HALF)
    lane = lax.broadcasted_iota(jnp.int32, (1, 2 * HALF), 1)
    column = lane & (HALF - 1)
    side = lax.broadcasted_iota(jnp.int32, whole, 1) & HALF
    sub = lax.broadcasted_iota(jnp.int32, (RANKS, 1), 0)
    pairs = list(pairs)
    for start in range(0, RANKS, panel):
        cols = [
            [
                jnp.take_along_axis(m, side + (start + j), axis=1, mode="promise_in_bounds")
                for j in range(panel)
            ]
            for m in pairs
        ]
        for j in range(panel):
            k = start + j
            for t in range(len(pairs)):
                a = pairs[t]
                col = cols[t][j]
                d = 1.0 / col[k : k + 1, :]
                row = jnp.where(column == k, d, a[k : k + 1, :] * d)
                for later in range(j + 1, panel):
                    factor = cols[t][later][k : k + 1, :] * d
                    cols[t][later] = jnp.where(
                        sub == k, factor, cols[t][later] - col * factor
                    )
                pairs[t] = jnp.where(
                    sub == k, row, jnp.where(column == k, 0.0, a) - col * row
                )
    return pairs


def compress_kernel(
    place, ids, ranks, low_hbm, got, h0, h1, h2, h3, y_out, c_out, err_out,
    low, sk, w_all, h_all, zt, cz, sems, low_sems,
):
    p, q, c = place[0], place[1], place[2]
    dot = functools.partial(jnp.dot, preferred_element_type=jnp.float32)

    def slot_of(k):
        return k, q < k * 8 + p

    def each(act):
        for k in range(SLOTS):
            a, active = slot_of(k)
            e = ids[a]

            fetch_entry(place, e, active, (h0, h1, h2, h3), sk.at[k], sems.at[k], act)

            @pl.when(active & ((e & 1) != c))
            def _(k=k, a=a):
                act(pltpu.make_async_copy(got.at[a], sk.at[k], sems.at[k]))

    each(lambda copy: copy.start())

    def load(k, act):
        for m in range(PARTS):
            part = pl.ds(m * (TILE // PARTS), TILE // PARTS)
            act(pltpu.make_async_copy(low_hbm.at[k, part], low.at[k, part], low_sems.at[k, m]))

    pl.when(slot_of(0)[1])(lambda: load(0, lambda copy: copy.start()))
    r2 = lax.broadcasted_iota(jnp.int32, (RANKS, RANKS), 0)
    c2 = lax.broadcasted_iota(jnp.int32, (RANKS, RANKS), 1)
    diag = r2 == c2
    for k in range(SLOTS):
        a, active = slot_of(k)

        @pl.when(jnp.logical_not(active))
        def _():
            y_out[a] = jnp.zeros((RANKS, TILE), jnp.float32)
            c_out[a] = jnp.zeros((RANKS, TILE), jnp.float32)
            h_all[k // 2, :, pl.ds(HALF * (k % 2), RANKS)] = jnp.where(diag, 1.0, 0.0)

    each(lambda copy: copy.wait())

    for k in range(SLOTS):
        a, active = slot_of(k)

        pl.when(active)(functools.partial(load, k, lambda copy: copy.wait()))
        if k + 1 < SLOTS:
            ahead = functools.partial(load, k + 1, lambda copy: copy.start())
            pl.when(slot_of(k + 1)[1])(ahead)

        @pl.when(active)
        def _(k=k, a=a):
            rank = ranks[a]
            row = lax.broadcasted_iota(jnp.int32, (RANKS, TILE), 0)
            chosen = jnp.where(row < rank, sk[k].astype(jnp.float32), 0.0).astype(jnp.bfloat16)
            sketched = dot_nt(chosen, low[k])
            y_out[a] = sketched
            parts = split3(sketched)
            w_all[k] = dot(parts[0], low[k])
            gram = three_pass(parts, parts, dot_nt)
            trace = jnp.sum(jnp.where(diag, gram, 0.0))
            mu = 0.1 * trace / rank.astype(jnp.float32)
            h_all[k // 2, :, pl.ds(HALF * (k % 2), RANKS)] = gram + jnp.where(
                diag, jnp.where(r2 < rank, mu, 1.0), 0.0
            )

    lanes = lax.broadcasted_iota(jnp.int32, (RANKS, 2 * HALF), 1)
    used = (lanes & (HALF - 1)) < RANKS
    pairs = [jnp.where(used, h_all[t], 0.0) for t in range(SLOTS // 2)]
    for t, inverse in enumerate(inverses(pairs, 8)):
        h_all[t] = inverse

    for k in range(SLOTS):
        a, active = slot_of(k)
        err_out[k] = jnp.zeros((8, 128), jnp.float32)

        @pl.when(active)
        def _(k=k, a=a):
            inverse = h_all[k // 2, :, pl.ds(HALF * (k % 2), RANKS)]
            coeffs = three_pass(split3(inverse), split3(w_all[k]), dot)
            c_out[a] = coeffs
            ch, cm, _unused = split3(coeffs)
            cz[...] = jnp.concatenate([ch, cm, ch], 0)
            yh, ym, _unused = split3(y_out[a])
            zt[...] = jnp.transpose(jnp.concatenate([yh, yh, ym], 0))
            acc = jnp.zeros((8, 128), jnp.float32)
            for n in range(4):
                lanes = slice(n * 256, (n + 1) * 256)
                approx = dot(zt[...], cz[:, lanes])
                rest = low[k, :, lanes].astype(jnp.float32) - approx
                rest = rest * rest
                rest = rest[:, :128] + rest[:, 128:]
                acc = acc + jnp.sum(rest.reshape(128, 8, 128), axis=0)
            err_out[k] = acc


def error_kernel(place, total, norms, errs, out, rank_out):
    p, q = place[0], place[1]
    summed = jnp.sum(total[...], axis=0)
    whole = jnp.sum(summed[0:1, :])
    lane = lax.broadcasted_iota(jnp.int32, (1, 128), 1)
    values = jnp.zeros((1, 128), jnp.float32)
    for k in range(SLOTS):
        i = k * 8 + p
        kept = jnp.where(q < i, jnp.sum(errs[k]), jnp.where(q == i, jnp.sum(norms[k]), 0.0))
        values = jnp.where(lane == k, kept, values)
    result = 32.0 * jnp.sqrt(values) / jnp.sqrt(jnp.full((1, 128), whole, jnp.float32))
    out[...] = result[:, :SLOTS]
    rank_out[0] = jnp.sum(summed[1:2, :]).astype(jnp.int32)


def covariance(*args):
    f32, bf16 = jnp.float32, jnp.bfloat16
    shape = jax.ShapeDtypeStruct
    return pl.pallas_call(
        covariance_kernel,
        out_shape=(
            shape((SLOTS, TILE, TILE), bf16),
            shape((SLOTS, 8, 128), f32),
            shape((1, 2, 128), f32),
        ),
        in_specs=[spec(SMEM)] * 4 + [spec(VMEM)] * 2,
        out_specs=[spec(pltpu.HBM)] + [spec(VMEM)] * 2,
        scratch_shapes=[
            VMEM((SLOTS, TILE, TILE), bf16),
            VMEM((128, 128), f32),
            VMEM((TILE, 128), f32),
            VMEM((TILE, 128), f32),
            pltpu.SemaphoreType.DMA((SLOTS,)),
        ],
        compiler_params=pltpu.CompilerParams(vmem_limit_bytes=50 << 20),
        cost_estimate=pl.CostEstimate(
            flops=100_000_000, bytes_accessed=8 << 20, transcendentals=8 << 20
        ),
        name="covariance",
    )(*args)


def compress(*args):
    f32, bf16 = jnp.float32, jnp.bfloat16
    shape = jax.ShapeDtypeStruct
    return pl.pallas_call(
        compress_kernel,
        out_shape=(
            shape((SLOTS, RANKS, TILE), f32),
            shape((SLOTS, RANKS, TILE), f32),
            shape((SLOTS, 8, 128), f32),
        ),
        in_specs=[spec(SMEM)] * 3 + [spec(pltpu.HBM)] + [spec(pl.ANY)] * 5,
        out_specs=[spec(VMEM)] * 3,
        scratch_shapes=[
            VMEM((SLOTS, TILE, TILE), bf16),
            VMEM((SLOTS, RANKS, TILE), bf16),
            VMEM((SLOTS, RANKS, TILE), f32),
            VMEM((SLOTS // 2, RANKS, 2 * HALF), f32),
            VMEM((TILE, 3 * RANKS), bf16),
            VMEM((3 * RANKS, TILE), bf16),
            pltpu.SemaphoreType.DMA((SLOTS,)),
            pltpu.SemaphoreType.DMA((SLOTS, PARTS)),
        ],
        compiler_params=pltpu.CompilerParams(vmem_limit_bytes=60 << 20),
        cost_estimate=pl.CostEstimate(
            flops=2_000_000_000, bytes_accessed=8 << 20, transcendentals=0
        ),
        name="compress",
    )(*args)


def device_program(points, range_length, smoothness, sketch_bank, sketch_ids, tile_ranks):
    f32, bf16, i32 = jnp.float32, jnp.bfloat16, jnp.int32
    shape = jax.ShapeDtypeStruct
    p = lax.axis_index("prow")
    y, x, c = (lax.axis_index(n) for n in PCOL)
    place = jnp.stack([p, (y * 4 + x) * 2 + c, c, y, x]).astype(i32)
    s = smoothness[0]
    factors = jnp.stack(
        [
            jnp.sqrt(2.0 * s.astype(f32) + 1.0) / range_length[0],
            jnp.float32(1.0 / 3.0),
        ]
    )
    ids = sketch_ids.reshape(SLOTS)
    ranks = tile_ranks.reshape(SLOTS)
    own = points.reshape(2, TILE)

    order = smoothness.astype(i32)
    rows = to_all(own, PCOL)
    held = bank_of_plane(sketch_bank[0])
    their_ids = swap_cores(ids)

    low, norms, share = covariance(place, order, factors, ranks, rows, own)

    theirs, again = pl.pallas_call(
        select_kernel,
        out_shape=(shape((SLOTS, RANKS, TILE), bf16), shape((256, 2, 128), f32)),
        in_specs=[spec(SMEM)] * 2 + [spec(VMEM)] + [spec(pl.ANY)] * 4,
        out_specs=[spec(VMEM)] * 2,
        scratch_shapes=[pltpu.SemaphoreType.DMA((SLOTS,))],
        compiler_params=pltpu.CompilerParams(vmem_limit_bytes=4 << 20),
        name="select",
    )(place, their_ids, share, *held)
    got = swap_cores(theirs)
    total = lax.all_to_all(again, ALL, split_axis=0, concat_axis=0)

    y_all, c_all, errs = compress(place, ids, ranks, low, got, *held)

    errors, rank_out = pl.pallas_call(
        error_kernel,
        out_shape=(shape((1, SLOTS), f32), shape((1,), i32)),
        in_specs=[spec(SMEM)] + [spec(VMEM)] * 3,
        out_specs=[spec(VMEM), spec(SMEM)],
        compiler_params=pltpu.CompilerParams(vmem_limit_bytes=4 << 20),
        name="errors",
    )(place, total, norms, errs)

    wide = (SLOTS, 1, 1, 1, RANKS, TILE)
    return (
        y_all.reshape(wide),
        c_all.reshape(wide),
        errors.reshape(SLOTS, 1, 1, 1),
        rank_out,
    )


def solution(mesh):
    split = Mesh(
        mesh.devices.reshape(mesh.shape["prow"], 4, 4, 2), ("prow", "pcol_0", "pcol_1", "pcol_2")
    )
    placed = (
        P(None, PCOL, None, None),
        P(),
        P(),
        P(PCOL, None, None),
        P(None, "prow", None, PCOL),
        P(None, "prow", None, PCOL),
    )
    return jax.shard_map(
        device_program,
        mesh=split,
        in_specs=placed,
        out_specs=(
            P(None, "prow", None, PCOL, None, None),
            P(None, "prow", None, PCOL, None, None),
            P(None, "prow", None, PCOL),
            P(),
        ),
        check_vma=False,
    )
```

```python
import functools

import jax
import jax.numpy as jnp
from jax import lax
from jax.experimental import pallas as pl
from jax.experimental.pallas import tpu as pltpu
from jax.sharding import Mesh
from jax.sharding import PartitionSpec as P


PCOL = ("pcol_0", "pcol_1", "pcol_2")
ALL = ("prow", "pcol_0", "pcol_1", "pcol_2")

TILE = 1024
RANKS = 48
SLOTS = 4
PARTS = 4
LOG2E = 1.4426950408889634
VMEM = pltpu.VMEM
SMEM = pltpu.SMEM


def spec(space):
    return pl.BlockSpec(memory_space=space)


def to_all(value, axes):
    copies = jnp.broadcast_to(value, (lax.axis_size(axes), *value.shape))
    return lax.all_to_all(copies, axes, split_axis=0, concat_axis=0)


def plane_shift(value, shift, stage):
    pairs = []
    for y in range(4):
        for x in range(4):
            for c in range(2):
                if (c == 0) == (stage == 0):
                    to = (y, (x + shift) % 4, c)
                else:
                    to = ((y + shift) % 4, x, c)
                pairs.append(((y * 4 + x) * 2 + c, (to[0] * 4 + to[1]) * 2 + to[2]))
    return lax.ppermute(value, PCOL, pairs)


def group_kernel(*refs):
    parts, out, sems = refs[:-2], refs[-2], refs[-1]
    moves = [pltpu.make_async_copy(part, out.at[i], sems.at[i]) for i, part in enumerate(parts)]
    for move in moves:
        move.start()
    for move in moves:
        move.wait()


def bank_of_plane(own):
    parts = [own] + [plane_shift(own, shift, 0) for shift in (1, 2, 3)]
    group = pl.pallas_call(
        group_kernel,
        out_shape=jax.ShapeDtypeStruct((4, *own.shape), own.dtype),
        in_specs=[spec(VMEM)] * 4,
        out_specs=spec(pltpu.HBM),
        scratch_shapes=[pltpu.SemaphoreType.DMA((4,))],
        compiler_params=pltpu.CompilerParams(vmem_limit_bytes=4 << 20),
        name="group_bank",
    )(*parts)
    return [group] + [plane_shift(group, shift, 1) for shift in (1, 2, 3)]


def fetch_entry(entry, wanted, held, out, sem, act):
    _, _, c, y, x = position()
    dy = (y - (entry >> 3)) & 3
    dx = (x - ((entry >> 1) & 3)) & 3
    inner = jnp.where(c == 0, dx, dy)
    outer = jnp.where(c == 0, dy, dx)
    for o in range(4):

        @pl.when(wanted & ((entry & 1) == c) & (outer == o))
        def _(o=o):
            act(pltpu.make_async_copy(held[o].at[inner], out, sem))


def swap_cores(value):
    return lax.ppermute(value, "pcol_2", [(0, 1), (1, 0)])


def position():
    y, x, c = (lax.axis_index(name) for name in PCOL)
    return lax.axis_index("prow"), (y * 4 + x) * 2 + c, c, y, x


def covariance_kernel(
    order, reach, ranks_hbm, rows, low_hbm, norms, share, low, turned, xb, yb, sems, ranks, ranks_sem
):
    bring = pltpu.make_async_copy(ranks_hbm, ranks, ranks_sem)
    bring.start()
    p, q, *_unused = position()
    wide = (16, 128)
    twice = jnp.full(wide, 2.0 * order[0].astype(jnp.float32) + 1.0, jnp.float32)
    scale = jnp.sqrt(twice) / jnp.full(wide, reach[0], jnp.float32)
    square = scale * scale * (1.0 / 3.0)
    power = scale * (-LOG2E)

    def tile(k, poly):
        points = rows[k * 8 + p]
        for g in range(8):
            turned[pl.ds(2 * g, 2), :] = points[:, g * 128 : (g + 1) * 128]
        columns = jnp.transpose(turned[...])
        for g in range(8):
            at = pl.ds(g * 128, 128)
            xb[at, :] = jnp.broadcast_to(columns[:, 2 * g : 2 * g + 1], (128, 128))
            yb[at, :] = jnp.broadcast_to(columns[:, 2 * g + 1 : 2 * g + 2], (128, 128))

        def strip(s, acc):
            at = pl.ds(pl.multiple_of(s * 16, 16), 16)
            xr = xb[at, :]
            yr = yb[at, :]
            for n in range(8):
                lanes = slice(n * 128, (n + 1) * 128)
                dx = xr - rows[q, 0:1, lanes]
                dy = yr - rows[q, 1:2, lanes]
                d2 = dx * dx + dy * dy
                r = d2 * lax.rsqrt(jnp.maximum(d2, 1e-30))
                v = poly(r, jnp.exp2(power * r))
                low[k, at, lanes] = v.astype(jnp.bfloat16)
                v2 = v * v
                acc = acc + (v2[0:8] + v2[8:16])
            return acc

        norms[k] = lax.fori_loop(0, 64, strip, jnp.zeros((8, 128), jnp.float32), unroll=2)

    polys = (
        lambda r, e: e,
        lambda r, e: (1.0 + scale * r) * e,
        lambda r, e: (1.0 + r * (scale + square * r)) * e,
    )

    def slot(k, acc):
        i = k * 8 + p
        norms[k] = jnp.zeros((8, 128), jnp.float32)
        for which in range(3):

            @pl.when((q <= i) & (order[0] == which))
            def _(which=which):
                tile(k, polys[which])

        @pl.when(q <= i)
        def _():
            pltpu.make_async_copy(low.at[k], low_hbm.at[k], sems.at[k]).start()

        acc = acc + jnp.where(q < i, 2.0, 1.0) * norms[k]
        return acc

    acc = lax.fori_loop(0, SLOTS, slot, jnp.zeros((8, 128), jnp.float32))
    bring.wait()
    rank_sum = jnp.int32(0)
    for k in range(SLOTS):
        rank_sum = rank_sum + jnp.where(q < k * 8 + p, ranks[k], 0)
    for k in range(SLOTS):

        @pl.when(q <= k * 8 + p)
        def _(k=k):
            pltpu.make_async_copy(low.at[k], low_hbm.at[k], sems.at[k]).wait()

    acc = jnp.sum(jnp.sum(acc, axis=0, keepdims=True), axis=1, keepdims=True)
    lane = lax.broadcasted_iota(jnp.int32, (1, 128), 1)
    both = jnp.where(lane == 0, acc, jnp.where(lane == 1, rank_sum.astype(jnp.float32), 0.0))
    share[...] = jnp.broadcast_to(both[None], share.shape)


def select_kernel(their_ids, h0, h1, h2, h3, theirs, sems):
    def each(act):
        for k in range(SLOTS):
            fetch_entry(their_ids[k], True, (h0, h1, h2, h3), theirs.at[k], sems.at[k], act)

    each(lambda copy: copy.start())
    each(lambda copy: copy.wait())


def split3(value):
    high = value.astype(jnp.bfloat16)
    rest = value - high.astype(jnp.float32)
    mid = rest.astype(jnp.bfloat16)
    return high, mid, (rest - mid.astype(jnp.float32)).astype(jnp.bfloat16)


def dot_nt(a, b, **kw):
    return lax.dot_general(
        a, b, (((1,), (1,)), ((), ())), preferred_element_type=jnp.float32, **kw
    )


def three_pass(parts_a, parts_b, dot):
    n = RANKS
    one = dot(jnp.concatenate(parts_a, 0), parts_b[0])
    two = dot(jnp.concatenate(parts_a[:2], 0), parts_b[1])
    three = dot(parts_a[0], parts_b[2])
    return one[0:n] + (one[n : 2 * n] + two[0:n]) + (one[2 * n :] + two[n:] + three)


HALF = 64


def inverses(pairs, panel):
    whole = (RANKS, 2 * HALF)
    lane = lax.broadcasted_iota(jnp.int32, (1, 2 * HALF), 1)
    column = lane & (HALF - 1)
    side = lax.broadcasted_iota(jnp.int32, whole, 1) & HALF
    sub = lax.broadcasted_iota(jnp.int32, (RANKS, 1), 0)
    pairs = list(pairs)
    for start in range(0, RANKS, panel):
        cols = [
            [
                jnp.take_along_axis(m, side + (start + j), axis=1, mode="promise_in_bounds")
                for j in range(panel)
            ]
            for m in pairs
        ]
        for j in range(panel):
            k = start + j
            for t in range(len(pairs)):
                a = pairs[t]
                col = cols[t][j]
                d = 1.0 / col[k : k + 1, :]
                row = jnp.where(column == k, d, a[k : k + 1, :] * d)
                for later in range(j + 1, panel):
                    factor = cols[t][later][k : k + 1, :] * d
                    cols[t][later] = jnp.where(
                        sub == k, factor, cols[t][later] - col * factor
                    )
                pairs[t] = jnp.where(
                    sub == k, row, jnp.where(column == k, 0.0, a) - col * row
                )
    return pairs


def compress_kernel(
    ids, ranks, norms, low_hbm, got, h0, h1, h2, h3, y_out, c_out, err_out,
    low, sk, w_all, h_all, zt, cz, sems, low_sems,
):
    p, q, c, *_unused = position()
    dot = functools.partial(jnp.dot, preferred_element_type=jnp.float32)

    def slot_of(k):
        return k, q < k * 8 + p

    def each(act):
        for k in range(SLOTS):
            a, active = slot_of(k)
            e = ids[a]

            fetch_entry(e, active, (h0, h1, h2, h3), sk.at[k], sems.at[k], act)

            @pl.when(active & ((e & 1) != c))
            def _(k=k, a=a):
                act(pltpu.make_async_copy(got.at[a], sk.at[k], sems.at[k]))

    each(lambda copy: copy.start())

    def load(k, act):
        for m in range(PARTS):
            part = pl.ds(m * (TILE // PARTS), TILE // PARTS)
            act(pltpu.make_async_copy(low_hbm.at[k, part], low.at[k, part], low_sems.at[k, m]))

    pl.when(slot_of(0)[1])(lambda: load(0, lambda copy: copy.start()))
    r2 = lax.broadcasted_iota(jnp.int32, (RANKS, RANKS), 0)
    c2 = lax.broadcasted_iota(jnp.int32, (RANKS, RANKS), 1)
    diag = r2 == c2
    for k in range(SLOTS):
        a, active = slot_of(k)

        @pl.when(jnp.logical_not(active))
        def _():
            y_out[a] = jnp.zeros((RANKS, TILE), jnp.float32)
            c_out[a] = jnp.zeros((RANKS, TILE), jnp.float32)
            h_all[k // 2, :, pl.ds(HALF * (k % 2), RANKS)] = jnp.where(diag, 1.0, 0.0)

    each(lambda copy: copy.wait())

    for k in range(SLOTS):
        a, active = slot_of(k)

        pl.when(active)(functools.partial(load, k, lambda copy: copy.wait()))
        if k + 1 < SLOTS:
            ahead = functools.partial(load, k + 1, lambda copy: copy.start())
            pl.when(slot_of(k + 1)[1])(ahead)

        @pl.when(active)
        def _(k=k, a=a):
            rank = ranks[a]
            row = lax.broadcasted_iota(jnp.int32, (RANKS, TILE), 0)
            chosen = jnp.where(row < rank, sk[k].astype(jnp.float32), 0.0).astype(jnp.bfloat16)
            sketched = dot_nt(chosen, low[k])
            y_out[a] = sketched
            parts = split3(sketched)
            w_all[k] = dot(parts[0], low[k])
            gram = three_pass(parts, parts, dot_nt)
            trace = jnp.sum(jnp.where(diag, gram, 0.0))
            mu = 0.1 * trace / rank.astype(jnp.float32)
            h_all[k // 2, :, pl.ds(HALF * (k % 2), RANKS)] = gram + jnp.where(
                diag, jnp.where(r2 < rank, mu, 1.0), 0.0
            )

    lanes = lax.broadcasted_iota(jnp.int32, (RANKS, 2 * HALF), 1)
    used = (lanes & (HALF - 1)) < RANKS
    pairs = [jnp.where(used, h_all[t], 0.0) for t in range(SLOTS // 2)]
    for t, inverse in enumerate(inverses(pairs, 8)):
        h_all[t] = inverse

    for k in range(SLOTS):
        a, active = slot_of(k)
        err_out[k] = jnp.where(q == k * 8 + p, norms[k], 0.0)

        @pl.when(active)
        def _(k=k, a=a):
            inverse = h_all[k // 2, :, pl.ds(HALF * (k % 2), RANKS)]
            coeffs = three_pass(split3(inverse), split3(w_all[k]), dot)
            c_out[a] = coeffs
            ch, cm, _unused = split3(coeffs)
            cz[...] = jnp.concatenate([ch, cm, ch], 0)
            yh, ym, _unused = split3(y_out[a])
            zt[...] = jnp.transpose(jnp.concatenate([yh, yh, ym], 0))
            acc = jnp.zeros((8, 128), jnp.float32)
            for n in range(4):
                lanes = slice(n * 256, (n + 1) * 256)
                approx = dot(zt[...], cz[:, lanes])
                rest = low[k, :, lanes].astype(jnp.float32) - approx
                rest = rest * rest
                rest = rest[:, :128] + rest[:, 128:]
                acc = acc + jnp.sum(rest.reshape(128, 8, 128), axis=0)
            err_out[k] = acc


def error_kernel(total, errs, out, rank_out):
    summed = jnp.sum(total[...], axis=0)
    whole = summed[:, 0:1]
    lane = lax.broadcasted_iota(jnp.int32, (1, 128), 1)
    values = jnp.zeros((1, 128), jnp.float32)
    for k in range(SLOTS):
        kept = jnp.sum(jnp.sum(errs[k], axis=0, keepdims=True), axis=1, keepdims=True)
        values = jnp.where(lane == k, kept, values)
    result = 32.0 * jnp.sqrt(values) / jnp.sqrt(whole)
    out[...] = result[:, :SLOTS]
    rank_out[0] = jnp.sum(summed[:, 1:2]).astype(jnp.int32)


def covariance(*args):
    f32, bf16 = jnp.float32, jnp.bfloat16
    shape = jax.ShapeDtypeStruct
    return pl.pallas_call(
        covariance_kernel,
        out_shape=(
            shape((SLOTS, TILE, TILE), bf16),
            shape((SLOTS, 8, 128), f32),
            shape((256, 1, 128), f32),
        ),
        in_specs=[spec(SMEM)] * 2 + [spec(pltpu.HBM), spec(VMEM)],
        out_specs=[spec(pltpu.HBM)] + [spec(VMEM)] * 2,
        scratch_shapes=[
            VMEM((SLOTS, TILE, TILE), bf16),
            VMEM((128, 128), f32),
            VMEM((TILE, 128), f32),
            VMEM((TILE, 128), f32),
            pltpu.SemaphoreType.DMA((SLOTS,)),
            SMEM((SLOTS,), jnp.int32),
            pltpu.SemaphoreType.DMA,
        ],
        compiler_params=pltpu.CompilerParams(vmem_limit_bytes=50 << 20),
        cost_estimate=pl.CostEstimate(
            flops=100_000_000, bytes_accessed=8 << 20, transcendentals=8 << 20
        ),
        name="covariance",
    )(*args)


def compress(*args):
    f32, bf16 = jnp.float32, jnp.bfloat16
    shape = jax.ShapeDtypeStruct
    return pl.pallas_call(
        compress_kernel,
        out_shape=(
            shape((SLOTS, RANKS, TILE), f32),
            shape((SLOTS, RANKS, TILE), f32),
            shape((SLOTS, 8, 128), f32),
        ),
        in_specs=[spec(SMEM)] * 2 + [spec(VMEM)] + [spec(pltpu.HBM), spec(VMEM)] + [spec(pl.ANY)] * 4,
        out_specs=[spec(VMEM)] * 3,
        scratch_shapes=[
            VMEM((SLOTS, TILE, TILE), bf16),
            VMEM((SLOTS, RANKS, TILE), bf16),
            VMEM((SLOTS, RANKS, TILE), f32),
            VMEM((SLOTS // 2, RANKS, 2 * HALF), f32),
            VMEM((TILE, 3 * RANKS), bf16),
            VMEM((3 * RANKS, TILE), bf16),
            pltpu.SemaphoreType.DMA((SLOTS,)),
            pltpu.SemaphoreType.DMA((SLOTS, PARTS)),
        ],
        compiler_params=pltpu.CompilerParams(vmem_limit_bytes=50 << 20),
        cost_estimate=pl.CostEstimate(
            flops=2_000_000_000, bytes_accessed=8 << 20, transcendentals=0
        ),
        name="compress",
    )(*args)


def device_program(points, range_length, smoothness, sketch_bank, sketch_ids, tile_ranks):
    f32, bf16, i32 = jnp.float32, jnp.bfloat16, jnp.int32
    shape = jax.ShapeDtypeStruct
    ids = sketch_ids.reshape(SLOTS)
    ranks = tile_ranks.reshape(SLOTS)
    own = points.reshape(2, TILE)

    rows = to_all(own, PCOL)
    held = bank_of_plane(sketch_bank[0])
    their_ids = swap_cores(ids)

    low, norms, share = covariance(smoothness, range_length, ranks, rows)

    theirs = pl.pallas_call(
        select_kernel,
        out_shape=shape((SLOTS, RANKS, TILE), bf16),
        in_specs=[spec(SMEM)] + [spec(pl.ANY)] * 4,
        out_specs=spec(VMEM),
        scratch_shapes=[pltpu.SemaphoreType.DMA((SLOTS,))],
        compiler_params=pltpu.CompilerParams(vmem_limit_bytes=4 << 20),
        name="select",
    )(their_ids, *held)
    got = swap_cores(theirs)
    total = lax.all_to_all(share, ALL, split_axis=0, concat_axis=0)

    y_all, c_all, errs = compress(ids, ranks, norms, low, got, *held)

    errors, rank_out = pl.pallas_call(
        error_kernel,
        out_shape=(shape((1, SLOTS), f32), shape((1,), i32)),
        in_specs=[spec(VMEM)] * 2,
        out_specs=[spec(VMEM), spec(SMEM)],
        compiler_params=pltpu.CompilerParams(vmem_limit_bytes=4 << 20),
        name="errors",
    )(total, errs)

    wide = (SLOTS, 1, 1, 1, RANKS, TILE)
    return (
        y_all.reshape(wide),
        c_all.reshape(wide),
        errors.reshape(SLOTS, 1, 1, 1),
        rank_out,
    )


def solution(mesh):
    split = Mesh(
        mesh.devices.reshape(mesh.shape["prow"], 4, 4, 2), ("prow", "pcol_0", "pcol_1", "pcol_2")
    )
    placed = (
        P(None, PCOL, None, None),
        P(),
        P(),
        P(PCOL, None, None),
        P(None, "prow", None, PCOL),
        P(None, "prow", None, PCOL),
    )
    return jax.shard_map(
        device_program,
        mesh=split,
        in_specs=placed,
        out_specs=(
            P(None, "prow", None, PCOL, None, None),
            P(None, "prow", None, PCOL, None, None),
            P(None, "prow", None, PCOL),
            P(),
        ),
        check_vma=False,
    )
```

```python
import functools

import jax
import jax.numpy as jnp
from jax import lax
from jax.experimental import pallas as pl
from jax.experimental.pallas import tpu as pltpu
from jax.sharding import Mesh
from jax.sharding import PartitionSpec as P


PCOL = ("pcol_0", "pcol_1", "pcol_2")
ALL = ("prow", "pcol_0", "pcol_1", "pcol_2")

TILE = 1024
RANKS = 48
SLOTS = 4
PARTS = 4
LOG2E = 1.4426950408889634
VMEM = pltpu.VMEM
SMEM = pltpu.SMEM


def spec(space):
    return pl.BlockSpec(memory_space=space)


def to_all(value, axes):
    copies = jnp.broadcast_to(value, (lax.axis_size(axes), *value.shape))
    return lax.all_to_all(copies, axes, split_axis=0, concat_axis=0)


def plane_shift(value, shift, stage):
    pairs = []
    for y in range(4):
        for x in range(4):
            for c in range(2):
                if (c == 0) == (stage == 0):
                    to = (y, (x + shift) % 4, c)
                else:
                    to = ((y + shift) % 4, x, c)
                pairs.append(((y * 4 + x) * 2 + c, (to[0] * 4 + to[1]) * 2 + to[2]))
    return lax.ppermute(value, PCOL, pairs)


def group_kernel(*refs):
    parts, out, sems = refs[:-2], refs[-2], refs[-1]
    moves = [pltpu.make_async_copy(part, out.at[i], sems.at[i]) for i, part in enumerate(parts)]
    for move in moves:
        move.start()
    for move in moves:
        move.wait()


def bank_of_plane(own):
    parts = [own] + [plane_shift(own, shift, 0) for shift in (1, 2, 3)]
    group = pl.pallas_call(
        group_kernel,
        out_shape=jax.ShapeDtypeStruct((4, *own.shape), own.dtype),
        in_specs=[spec(VMEM)] * 4,
        out_specs=spec(pltpu.HBM),
        scratch_shapes=[pltpu.SemaphoreType.DMA((4,))],
        compiler_params=pltpu.CompilerParams(vmem_limit_bytes=4 << 20),
        name="group_bank",
    )(*parts)
    return [group] + [plane_shift(group, shift, 1) for shift in (1, 2, 3)]


def fetch_entry(entry, wanted, held, out, sem, act):
    _, _, c, y, x = position()
    dy = (y - (entry >> 3)) & 3
    dx = (x - ((entry >> 1) & 3)) & 3
    inner = jnp.where(c == 0, dx, dy)
    outer = jnp.where(c == 0, dy, dx)
    for o in range(4):

        @pl.when(wanted & ((entry & 1) == c) & (outer == o))
        def _(o=o):
            act(pltpu.make_async_copy(held[o].at[inner], out, sem))


def swap_cores(value):
    return lax.ppermute(value, "pcol_2", [(0, 1), (1, 0)])


def position():
    y, x, c = (lax.axis_index(name) for name in PCOL)
    return lax.axis_index("prow"), (y * 4 + x) * 2 + c, c, y, x


def covariance_kernel(
    order, reach, ranks_hbm, rows, low_hbm, norms, share, low, turned, xb, yb, sems, ranks, ranks_sem
):
    bring = pltpu.make_async_copy(ranks_hbm, ranks, ranks_sem)
    bring.start()
    p, q, *_unused = position()
    wide = (16, 128)
    twice = jnp.full(wide, 2.0 * order[0].astype(jnp.float32) + 1.0, jnp.float32)
    scale = jnp.sqrt(twice) / jnp.full(wide, reach[0], jnp.float32)
    square = scale * scale * (1.0 / 3.0)
    power = scale * (-LOG2E)

    def tile(k, poly):
        points = rows[k * 8 + p]
        for g in range(8):
            turned[pl.ds(2 * g, 2), :] = points[:, g * 128 : (g + 1) * 128]
        columns = jnp.transpose(turned[...])
        for g in range(8):
            at = pl.ds(g * 128, 128)
            xb[at, :] = jnp.broadcast_to(columns[:, 2 * g : 2 * g + 1], (128, 128))
            yb[at, :] = jnp.broadcast_to(columns[:, 2 * g + 1 : 2 * g + 2], (128, 128))

        def strip(s, acc):
            at = pl.ds(pl.multiple_of(s * 16, 16), 16)
            xr = xb[at, :]
            yr = yb[at, :]
            for n in range(8):
                lanes = slice(n * 128, (n + 1) * 128)
                dx = xr - rows[q, 0:1, lanes]
                dy = yr - rows[q, 1:2, lanes]
                d2 = dx * dx + dy * dy
                r = d2 * lax.rsqrt(jnp.maximum(d2, 1e-30))
                v = poly(r, jnp.exp2(power * r))
                low[k, at, lanes] = v.astype(jnp.bfloat16)
                v2 = v * v
                acc = acc + (v2[0:8] + v2[8:16])
            return acc

        norms[k] = lax.fori_loop(0, 64, strip, jnp.zeros((8, 128), jnp.float32), unroll=2)

    polys = (
        lambda r, e: e,
        lambda r, e: (1.0 + scale * r) * e,
        lambda r, e: (1.0 + r * (scale + square * r)) * e,
    )

    def slot(k, acc):
        i = k * 8 + p
        norms[k] = jnp.zeros((8, 128), jnp.float32)
        for which in range(3):

            @pl.when((q <= i) & (order[0] == which))
            def _(which=which):
                tile(k, polys[which])

        @pl.when(q <= i)
        def _():
            pltpu.make_async_copy(low.at[k], low_hbm.at[k], sems.at[k]).start()

        acc = acc + jnp.where(q < i, 2.0, 1.0) * norms[k]
        return acc

    acc = lax.fori_loop(0, SLOTS, slot, jnp.zeros((8, 128), jnp.float32))
    bring.wait()
    rank_sum = jnp.int32(0)
    for k in range(SLOTS):
        rank_sum = rank_sum + jnp.where(q < k * 8 + p, ranks[k], 0)
    for k in range(SLOTS):

        @pl.when(q <= k * 8 + p)
        def _(k=k):
            pltpu.make_async_copy(low.at[k], low_hbm.at[k], sems.at[k]).wait()

    acc = jnp.sum(jnp.sum(acc, axis=0, keepdims=True), axis=1, keepdims=True)
    lane = lax.broadcasted_iota(jnp.int32, (1, 128), 1)
    both = jnp.where(lane == 0, acc, jnp.where(lane == 1, rank_sum.astype(jnp.float32), 0.0))
    share[...] = jnp.broadcast_to(both[None], share.shape)


def select_kernel(their_ids, h0, h1, h2, h3, theirs, sems):
    def each(act):
        for k in range(SLOTS):
            fetch_entry(their_ids[k], True, (h0, h1, h2, h3), theirs.at[k], sems.at[k], act)

    each(lambda copy: copy.start())
    each(lambda copy: copy.wait())


def split3(value):
    high = value.astype(jnp.bfloat16)
    rest = value - high.astype(jnp.float32)
    mid = rest.astype(jnp.bfloat16)
    return high, mid, (rest - mid.astype(jnp.float32)).astype(jnp.bfloat16)


def dot_nt(a, b, **kw):
    return lax.dot_general(
        a, b, (((1,), (1,)), ((), ())), preferred_element_type=jnp.float32, **kw
    )


def three_pass(parts_a, parts_b, dot):
    n = RANKS
    one = dot(jnp.concatenate(parts_a, 0), parts_b[0])
    two = dot(jnp.concatenate(parts_a[:2], 0), parts_b[1])
    three = dot(parts_a[0], parts_b[2])
    return one[0:n] + (one[n : 2 * n] + two[0:n]) + (one[2 * n :] + two[n:] + three)


HALF = 64


def inverses(pairs, panel):
    whole = (RANKS, 2 * HALF)
    lane = lax.broadcasted_iota(jnp.int32, (1, 2 * HALF), 1)
    column = lane & (HALF - 1)
    side = lax.broadcasted_iota(jnp.int32, whole, 1) & HALF
    sub = lax.broadcasted_iota(jnp.int32, (RANKS, 1), 0)
    pairs = list(pairs)
    for start in range(0, RANKS, panel):
        cols = [
            [
                jnp.take_along_axis(m, side + (start + j), axis=1, mode="promise_in_bounds")
                for j in range(panel)
            ]
            for m in pairs
        ]
        for j in range(panel):
            k = start + j
            for t in range(len(pairs)):
                a = pairs[t]
                col = cols[t][j]
                d = 1.0 / col[k : k + 1, :]
                row = jnp.where(column == k, d, a[k : k + 1, :] * d)
                for later in range(j + 1, panel):
                    factor = cols[t][later][k : k + 1, :] * d
                    cols[t][later] = jnp.where(
                        sub == k, factor, cols[t][later] - col * factor
                    )
                pairs[t] = jnp.where(
                    sub == k, row, jnp.where(column == k, 0.0, a) - col * row
                )
    return pairs


def compress_kernel(
    ids, ranks, norms, low_hbm, got, h0, h1, h2, h3, y_out, c_out, err_out,
    low, sk, w_all, h_all, zt, cz, sems, low_sems,
):
    p, q, c, *_unused = position()
    dot = functools.partial(jnp.dot, preferred_element_type=jnp.float32)

    def slot_of(k):
        return k, q < k * 8 + p

    def each(act):
        for k in range(SLOTS):
            a, active = slot_of(k)
            e = ids[a]

            fetch_entry(e, active, (h0, h1, h2, h3), sk.at[k], sems.at[k], act)

            @pl.when(active & ((e & 1) != c))
            def _(k=k, a=a):
                act(pltpu.make_async_copy(got.at[a], sk.at[k], sems.at[k]))

    each(lambda copy: copy.start())

    def load(k, act):
        for m in range(PARTS):
            part = pl.ds(m * (TILE // PARTS), TILE // PARTS)
            act(pltpu.make_async_copy(low_hbm.at[k, part], low.at[k, part], low_sems.at[k, m]))

    pl.when(slot_of(0)[1])(lambda: load(0, lambda copy: copy.start()))
    r2 = lax.broadcasted_iota(jnp.int32, (RANKS, RANKS), 0)
    c2 = lax.broadcasted_iota(jnp.int32, (RANKS, RANKS), 1)
    diag = r2 == c2
    for k in range(SLOTS):
        a, active = slot_of(k)

        @pl.when(jnp.logical_not(active))
        def _():
            y_out[a] = jnp.zeros((RANKS, TILE), jnp.float32)
            c_out[a] = jnp.zeros((RANKS, TILE), jnp.float32)
            h_all[k // 2, :, pl.ds(HALF * (k % 2), RANKS)] = jnp.where(diag, 1.0, 0.0)

    each(lambda copy: copy.wait())

    for k in range(SLOTS):
        a, active = slot_of(k)

        if k > 0:
            pl.when(active)(functools.partial(load, k, lambda copy: copy.wait()))
        if k + 1 < SLOTS:
            ahead = functools.partial(load, k + 1, lambda copy: copy.start())
            later = slot_of(k + 1)[1]
            pl.when(later & jnp.logical_not(active) if k == 0 else later)(ahead)

        @pl.when(active)
        def _(k=k, a=a):
            rank = ranks[a]
            row = lax.broadcasted_iota(jnp.int32, (RANKS, TILE), 0)
            chosen = jnp.where(row < rank, sk[k].astype(jnp.float32), 0.0).astype(jnp.bfloat16)
            if k == 0:
                pieces = []
                for m in range(PARTS):
                    part = pl.ds(m * (TILE // PARTS), TILE // PARTS)
                    pltpu.make_async_copy(
                        low_hbm.at[0, part], low.at[0, part], low_sems.at[0, m]
                    ).wait()
                    pieces.append(dot_nt(chosen, low[0, part, :]))
                load(1, lambda copy: copy.start())
                sketched = jnp.concatenate(pieces, 1)
            else:
                sketched = dot_nt(chosen, low[k])
            y_out[a] = sketched
            parts = split3(sketched)
            w_all[k] = dot(parts[0], low[k])
            gram = three_pass(parts, parts, dot_nt)
            trace = jnp.sum(jnp.where(diag, gram, 0.0))
            mu = 0.1 * trace / rank.astype(jnp.float32)
            h_all[k // 2, :, pl.ds(HALF * (k % 2), RANKS)] = gram + jnp.where(
                diag, jnp.where(r2 < rank, mu, 1.0), 0.0
            )

    lanes = lax.broadcasted_iota(jnp.int32, (RANKS, 2 * HALF), 1)
    used = (lanes & (HALF - 1)) < RANKS
    pairs = [jnp.where(used, h_all[t], 0.0) for t in range(SLOTS // 2)]
    for t, inverse in enumerate(inverses(pairs, 8)):
        h_all[t] = inverse

    for k in range(SLOTS):
        a, active = slot_of(k)
        err_out[k] = jnp.where(q == k * 8 + p, norms[k], 0.0)

        @pl.when(active)
        def _(k=k, a=a):
            inverse = h_all[k // 2, :, pl.ds(HALF * (k % 2), RANKS)]
            coeffs = three_pass(split3(inverse), split3(w_all[k]), dot)
            c_out[a] = coeffs
            ch, cm, _unused = split3(coeffs)
            cz[...] = jnp.concatenate([ch, cm, ch], 0)
            yh, ym, _unused = split3(y_out[a])
            zt[...] = jnp.transpose(jnp.concatenate([yh, yh, ym], 0))
            acc = jnp.zeros((8, 128), jnp.float32)
            for n in range(4):
                lanes = slice(n * 256, (n + 1) * 256)
                approx = dot(zt[...], cz[:, lanes])
                rest = low[k, :, lanes].astype(jnp.float32) - approx
                rest = rest * rest
                rest = rest[:, :128] + rest[:, 128:]
                acc = acc + jnp.sum(rest.reshape(128, 8, 128), axis=0)
            err_out[k] = acc


def error_kernel(total, errs, out, rank_out):
    summed = jnp.sum(total[...], axis=0)
    whole = summed[:, 0:1]
    lane = lax.broadcasted_iota(jnp.int32, (1, 128), 1)
    values = jnp.zeros((1, 128), jnp.float32)
    for k in range(SLOTS):
        kept = jnp.sum(jnp.sum(errs[k], axis=0, keepdims=True), axis=1, keepdims=True)
        values = jnp.where(lane == k, kept, values)
    result = 32.0 * jnp.sqrt(values) / jnp.sqrt(whole)
    out[...] = result[:, :SLOTS]
    rank_out[0] = jnp.sum(summed[:, 1:2]).astype(jnp.int32)


def covariance(*args):
    f32, bf16 = jnp.float32, jnp.bfloat16
    shape = jax.ShapeDtypeStruct
    return pl.pallas_call(
        covariance_kernel,
        out_shape=(
            shape((SLOTS, TILE, TILE), bf16),
            shape((SLOTS, 8, 128), f32),
            shape((256, 1, 128), f32),
        ),
        in_specs=[spec(SMEM)] * 2 + [spec(pltpu.HBM), spec(VMEM)],
        out_specs=[spec(pltpu.HBM)] + [spec(VMEM)] * 2,
        scratch_shapes=[
            VMEM((SLOTS, TILE, TILE), bf16),
            VMEM((128, 128), f32),
            VMEM((TILE, 128), f32),
            VMEM((TILE, 128), f32),
            pltpu.SemaphoreType.DMA((SLOTS,)),
            SMEM((SLOTS,), jnp.int32),
            pltpu.SemaphoreType.DMA,
        ],
        compiler_params=pltpu.CompilerParams(vmem_limit_bytes=50 << 20),
        cost_estimate=pl.CostEstimate(
            flops=100_000_000, bytes_accessed=8 << 20, transcendentals=8 << 20
        ),
        name="covariance",
    )(*args)


def compress(*args):
    f32, bf16 = jnp.float32, jnp.bfloat16
    shape = jax.ShapeDtypeStruct
    return pl.pallas_call(
        compress_kernel,
        out_shape=(
            shape((SLOTS, RANKS, TILE), f32),
            shape((SLOTS, RANKS, TILE), f32),
            shape((SLOTS, 8, 128), f32),
        ),
        in_specs=[spec(SMEM)] * 2 + [spec(VMEM)] + [spec(pltpu.HBM), spec(VMEM)] + [spec(pl.ANY)] * 4,
        out_specs=[spec(VMEM)] * 3,
        scratch_shapes=[
            VMEM((SLOTS, TILE, TILE), bf16),
            VMEM((SLOTS, RANKS, TILE), bf16),
            VMEM((SLOTS, RANKS, TILE), f32),
            VMEM((SLOTS // 2, RANKS, 2 * HALF), f32),
            VMEM((TILE, 3 * RANKS), bf16),
            VMEM((3 * RANKS, TILE), bf16),
            pltpu.SemaphoreType.DMA((SLOTS,)),
            pltpu.SemaphoreType.DMA((SLOTS, PARTS)),
        ],
        compiler_params=pltpu.CompilerParams(vmem_limit_bytes=50 << 20),
        cost_estimate=pl.CostEstimate(
            flops=2_000_000_000, bytes_accessed=8 << 20, transcendentals=0
        ),
        name="compress",
    )(*args)


def device_program(points, range_length, smoothness, sketch_bank, sketch_ids, tile_ranks):
    f32, bf16, i32 = jnp.float32, jnp.bfloat16, jnp.int32
    shape = jax.ShapeDtypeStruct
    ids = sketch_ids.reshape(SLOTS)
    ranks = tile_ranks.reshape(SLOTS)
    own = points.reshape(2, TILE)

    rows = to_all(own, PCOL)
    held = bank_of_plane(sketch_bank[0])
    their_ids = swap_cores(ids)

    low, norms, share = covariance(smoothness, range_length, ranks, rows)

    theirs = pl.pallas_call(
        select_kernel,
        out_shape=shape((SLOTS, RANKS, TILE), bf16),
        in_specs=[spec(SMEM)] + [spec(pl.ANY)] * 4,
        out_specs=spec(VMEM),
        scratch_shapes=[pltpu.SemaphoreType.DMA((SLOTS,))],
        compiler_params=pltpu.CompilerParams(vmem_limit_bytes=4 << 20),
        name="select",
    )(their_ids, *held)
    got = swap_cores(theirs)
    total = lax.all_to_all(share, ALL, split_axis=0, concat_axis=0)

    y_all, c_all, errs = compress(ids, ranks, norms, low, got, *held)

    errors, rank_out = pl.pallas_call(
        error_kernel,
        out_shape=(shape((1, SLOTS), f32), shape((1,), i32)),
        in_specs=[spec(VMEM)] * 2,
        out_specs=[spec(VMEM), spec(SMEM)],
        compiler_params=pltpu.CompilerParams(vmem_limit_bytes=4 << 20),
        name="errors",
    )(total, errs)

    wide = (SLOTS, 1, 1, 1, RANKS, TILE)
    return (
        y_all.reshape(wide),
        c_all.reshape(wide),
        errors.reshape(SLOTS, 1, 1, 1),
        rank_out,
    )


def solution(mesh):
    split = Mesh(
        mesh.devices.reshape(mesh.shape["prow"], 4, 4, 2), ("prow", "pcol_0", "pcol_1", "pcol_2")
    )
    placed = (
        P(None, PCOL, None, None),
        P(),
        P(),
        P(PCOL, None, None),
        P(None, "prow", None, PCOL),
        P(None, "prow", None, PCOL),
    )
    return jax.shard_map(
        device_program,
        mesh=split,
        in_specs=placed,
        out_specs=(
            P(None, "prow", None, PCOL, None, None),
            P(None, "prow", None, PCOL, None, None),
            P(None, "prow", None, PCOL),
            P(),
        ),
        check_vma=False,
    )
```
